128 devices in a mesh: dp: 2 (over core), seq: 16 (over y, x), tensor: 4 (over z).
Axes of the slice: x: 4, y: 4, z: 4, core: 2. Of those that a mesh axis runs over, the one named last changes fastest.
Arguments:
- tokens: bfloat16 [2, 8192, 2048], P('dp', ('seq', 'tensor')), may hold values from -6 to 6
- attn_gain: float32 [2048], replicated, may hold values from 0.5 to 1.5
- w_qkv: bfloat16 [3, 2048, 2048], P(None, None, 'tensor'), may hold values from -1 to 1
- w_out: bfloat16 [2048, 2048], P('tensor'), may hold values from -0.125 to 0.125
- mlp_gain: float32 [2048], replicated, may hold values from 0.5 to 1.5
- w_up: bfloat16 [2048, 8192], P(None, 'tensor'), may hold values from -0.125 to 0.125
- w_down: bfloat16 [8192, 2048], P('tensor'), may hold values from -0.0625 to 0.0625
- pool_gain: float32 [2048], replicated, may hold values from -8 to 8
- pool_bias: float32 [2048], replicated, may hold values from 0.5 to 5
- value_weight: float32 [2048], replicated, may hold values from -6 to 6
- valid_frames: int32 [2], replicated, may hold values from 16 to 32, as said below
Outputs:
- hidden: bfloat16 [2, 8192, 2048], P('dp', ('seq', 'tensor'))
- frame_values: float32 [2, 32], P('dp', 'seq')
- advantages: float32 [2, 32], P('dp', 'seq')
The draws below stay inside these ranges and needn't reach their ends.
Inputs may be any that keep to these rules, and one draw needn't show every extreme that they name: `valid_frames`: at least one rollout keeps all 32 frames and at least one keeps 32 // 2 of them.
All inputs are finite; a program needn't handle non-finite values.
Results may differ from the reference program's by a relative error of at most 0.017.
Values may be sent and summed in bfloat16 or wider, within the bound.
No kernel may reach another device: no remote copies, remote signals or barrier semaphores. Data moves between devices by JAX's collectives and lax.ppermute only.
A program may use at most 256 MiB of HBM per device.

```python
import jax
import jax.numpy as jnp
from jax import lax

D = 2048
HEADS = 16
HEAD_DIM = 128
FF = 8192
TOK_FRAME = 256
FRAMES = 32
TOKENS = 8192
ROLLOUTS = 2


def draw_tokens(key, part):
    noise_key = jax.random.fold_in(key, 11)
    values = jax.random.truncated_normal(noise_key, -6.0, 6.0, (ROLLOUTS, TOKENS, D), jnp.float32)
    return values.astype(jnp.bfloat16)


def draw_w_qkv(key, part):
    base = jax.random.truncated_normal(jax.random.fold_in(key, 21), -6.0, 6.0, (3, D, D), jnp.float32) / jnp.sqrt(jnp.float32(D))
    return base.astype(jnp.bfloat16)


def draw_valid_frames(key, part):
    base = jax.random.randint(jax.random.fold_in(key, 31), (ROLLOUTS,), FRAMES // 2, FRAMES + 1, dtype=jnp.int32)
    rank = jax.random.permutation(jax.random.fold_in(key, 32), jnp.arange(ROLLOUTS, dtype=jnp.int32))
    longest = jnp.full((ROLLOUTS,), FRAMES, jnp.int32)
    shortest = jnp.full((ROLLOUTS,), FRAMES // 2, jnp.int32)
    return jnp.where(rank == 0, longest, jnp.where(rank == 1, shortest, base)).astype(jnp.int32)


def shard_levels(stream_key, shape, split, least, high):
    level = 1.0
    for dim, parts in split:
        heights = jax.random.uniform(jax.random.fold_in(jax.random.fold_in(stream_key, 6), dim), (parts,), jnp.float32, least / len(split), high / len(split))
        level = level * jnp.repeat(jnp.exp(heights), shape[dim] // parts).reshape((-1,) + (1,) * (len(shape) - 1 - dim))
    return level


def normal_values(rng, dims, scale, reach, shards=(), held_as=jnp.bfloat16):
    array = scale * jax.random.normal(rng, dims, jnp.float32)
    if shards:
        array = array * shard_levels(rng, dims, shards, -0.22, 0.18)
    return jnp.clip(array, -reach, reach).astype(held_as)


def setup_inputs(seed: int = 0) -> dict:
    key_list = jax.random.split(jax.random.key(seed), 12)
    tokens = draw_tokens(jax.random.fold_in(key_list[11], 71), 0)
    attn_gain = jnp.clip(1.0 + 0.1 * jax.random.normal(key_list[1], (D,), jnp.float32), 0.5, 1.5)
    w_qkv = draw_w_qkv(jax.random.fold_in(key_list[11], 71), 0)
    w_out = normal_values(key_list[3], (D, D), D ** -0.5, 0.125, ((0, 4),))
    mlp_gain = jnp.clip(1.0 + 0.1 * jax.random.normal(key_list[4], (D,), jnp.float32), 0.5, 1.5)
    w_up = normal_values(key_list[5], (D, FF), D ** -0.5, 0.125, ((1, 4),))
    w_down = normal_values(key_list[6], (FF, D), FF ** -0.5, 0.0625, ((0, 4),))
    pool_gain = jnp.clip(jax.random.uniform(key_list[7], (D,), jnp.float32, -8.0, 8.0), -8.0, 8.0)
    pool_bias = jnp.clip(jax.random.uniform(key_list[8], (D,), jnp.float32, 0.5, 5.0), 0.5, 5.0)
    value_weight = normal_values(key_list[9], (D,), 1.0, 6.0, (), jnp.float32)
    valid_frames = draw_valid_frames(jax.random.fold_in(key_list[11], 71), 0)
    return dict(tokens=tokens, attn_gain=attn_gain, w_qkv=w_qkv, w_out=w_out, mlp_gain=mlp_gain, w_up=w_up, w_down=w_down, pool_gain=pool_gain, pool_bias=pool_bias, value_weight=value_weight, valid_frames=valid_frames)


def rms_norm(values, gain):
    floats = values.astype(jnp.float32)
    square = lax.optimization_barrier(jnp.mean(floats * floats, axis=-1, keepdims=True))
    return (floats * lax.rsqrt(square + 1e-05) * gain).astype(jnp.bfloat16)

def reference(tokens, attn_gain, w_qkv, w_out, mlp_gain, w_up, w_down, pool_gain, pool_bias, value_weight, valid_frames):
    scale = 1.0 / HEAD_DIM ** 0.5
    frame_of = jnp.arange(TOKENS, dtype=jnp.int32) // TOK_FRAME

    def layer(args):
        rows, length = args
        normed = rms_norm(rows, attn_gain)
        qkv = jnp.einsum('nd,cde->nce', normed.astype(jnp.float32), w_qkv.astype(jnp.float32)).astype(jnp.bfloat16)
        query = qkv[:, 0].reshape(TOKENS, HEADS, HEAD_DIM).transpose(1, 0, 2)
        keys = qkv[:, 1].reshape(TOKENS, HEADS, HEAD_DIM).transpose(1, 0, 2)
        vals = qkv[:, 2].reshape(TOKENS, HEADS, HEAD_DIM).transpose(1, 0, 2)
        allowed = (frame_of[None, :] <= frame_of[:, None]) & (frame_of[None, :] < length)

        def head(trio):
            qh, kh, vh = trio
            scores = jnp.dot(qh, kh.T, preferred_element_type=jnp.float32) * scale
            scores = jnp.where(allowed, scores, -1e+30)
            peak = lax.optimization_barrier(jnp.max(scores, axis=-1, keepdims=True))
            weights = jnp.where(allowed, jnp.exp(scores - peak), 0.0)
            total = lax.optimization_barrier(jnp.sum(weights, axis=-1, keepdims=True))
            numer = jnp.dot(weights.astype(jnp.bfloat16), vh, preferred_element_type=jnp.float32)
            return numer / total
        mixed = lax.map(head, (query, keys, vals)).transpose(1, 0, 2).reshape(TOKENS, D).astype(jnp.bfloat16)
        after_attn = (rows.astype(jnp.float32) + jnp.dot(mixed, w_out, preferred_element_type=jnp.float32)).astype(jnp.bfloat16)
        normed2 = rms_norm(after_attn, mlp_gain)
        up = jax.nn.gelu(jnp.dot(normed2, w_up, preferred_element_type=jnp.float32), approximate=True).astype(jnp.bfloat16)
        return (after_attn.astype(jnp.float32) + jnp.dot(up, w_down, preferred_element_type=jnp.float32)).astype(jnp.bfloat16)
    hidden = lax.map(layer, (tokens, valid_frames))
    means = lax.optimization_barrier(jnp.mean(hidden.astype(jnp.float32).reshape(ROLLOUTS, FRAMES, TOK_FRAME, D), axis=2))
    frame_ids = jnp.arange(FRAMES, dtype=jnp.int32)
    valid = frame_ids[None, :] < valid_frames[:, None]

    def advance(state, inputs):
        mean_f, valid_f = inputs
        gate = jax.nn.sigmoid(mean_f * pool_gain + pool_bias)
        new = gate * state + (1.0 - gate) * mean_f
        state = jnp.where(valid_f[:, None], new, state)
        return (state, state)
    start = jnp.zeros((ROLLOUTS, D), jnp.float32)
    _, states = lax.scan(advance, start, (means.transpose(1, 0, 2), valid.T))
    states = states.transpose(1, 0, 2)
    frame_values = jnp.where(valid, lax.optimization_barrier(jnp.sum(states * value_weight, axis=-1)), 0.0)
    last = frame_ids[None, :] == valid_frames[:, None] - 1
    reward = lax.optimization_barrier(jnp.sum(jnp.where(last, frame_values, 0.0), axis=1))
    gap = jnp.where(valid, reward[:, None] - frame_values, 0.0)
    count = jnp.sum(valid_frames).astype(jnp.float32)
    mean = jnp.sum(gap) / count
    centered = jnp.where(valid, gap - mean, 0.0)
    variance = jnp.sum(centered * centered) / count
    advantages = jnp.where(valid, centered * lax.rsqrt(variance + 1e-05), 0.0)
    return (hidden, frame_values, advantages)
```

```python
import functools
import math

import jax
import jax.numpy as jnp
from jax import lax
from jax.experimental import pallas as pl
from jax.experimental.pallas import tpu as pltpu
from jax.sharding import Mesh, PartitionSpec as P

D = 2048
HD = 128
QT = 128
FRAMES = 32
TOK_FRAME = 256
BF = jnp.bfloat16
F32 = jnp.float32
QSCALE = math.log2(math.e) / math.sqrt(HD)
SHIFTS = (0, -1, 1, 2)
VMEM = pltpu.VMEM
SMEM = pltpu.SMEM


def ring(shift):
    return [(i, (i + shift) % 4) for i in range(4)]


def moved(array, axis, shift):
    return lax.ppermute(array, axis, ring(shift))


def flat(*digits):
    sizes = {2: (2, 4), 3: (2, 4, 4)}[len(digits)]
    at = 0
    for digit, size in zip(digits, sizes):
        at = at * size + digit
    return at


def seats():
    return tuple(lax.axis_index(name).astype(jnp.int32) for name in ("dp", "y", "x", "tensor"))


def call(body, out, ins, scratch=(), grid=None, in_specs=None, out_specs=None, flops=0, size=0, limit=None):
    single = not isinstance(out, (list, tuple))
    outs = [out] if single else list(out)
    whole = pl.BlockSpec(memory_space=VMEM)
    kwargs = {} if grid is None else {"grid": grid}
    return pl.pallas_call(
        body,
        out_shape=out if single else outs,
        in_specs=in_specs or [whole] * len(ins),
        out_specs=out_specs or (whole if single else [whole] * len(outs)),
        scratch_shapes=list(scratch),
        compiler_params=pltpu.CompilerParams(vmem_limit_bytes=limit),
        cost_estimate=pl.CostEstimate(flops=flops, bytes_accessed=size, transcendentals=0),
        **kwargs,
    )(*ins)


def shape(dims, kind=BF):
    return jax.ShapeDtypeStruct(tuple(dims), kind)


def normalized(floats, gain):
    square = jnp.mean(floats * floats, axis=-1, keepdims=True)
    return (floats * lax.rsqrt(square + 1e-05) * gain).astype(BF)


def qkv_body(parts, gain, *refs):
    place = seats()
    rows, w, outs, normed, made = refs[:parts], refs[parts], refs[parts + 1 : parts + 5], refs[-2], refs[-1]
    step = pl.program_id(0)

    @pl.when(step == 0)
    def _():
        at = 0
        for part in rows:
            n = part.shape[0]
            normed[at : at + n, :] = normalized(part[...].astype(F32), gain[...])
            at += n

    product = jnp.dot(normed[...], w[0], preferred_element_type=F32)
    product = product * jnp.where(step == 0, QSCALE, 1.0)
    made[...] = product.astype(BF)
    slot = lax.rem(step + 2, 3)
    for rel in range(4):
        head = lax.rem(place[2] + rel, 4)
        outs[rel][:, pl.ds(pl.multiple_of(slot * HD, HD), HD)] = made[:, pl.ds(pl.multiple_of(head * HD, HD), HD)]


def qkv_of(gain, parts, w):
    n = sum(part.shape[0] for part in parts)
    whole = lambda dims: pl.BlockSpec(tuple(dims), lambda c: (0,) * len(dims))
    return call(
        functools.partial(qkv_body, len(parts)),
        [shape((n, 3 * HD))] * 4,
        [gain, *parts, w],
        [pltpu.VMEM((n, D), BF), pltpu.VMEM((n, 4 * HD), BF)],
        grid=(3,),
        in_specs=[whole((1, D)), *(whole(part.shape) for part in parts),
                  pl.BlockSpec((1, D, 4 * HD), lambda c: (c, 0, 0))],
        out_specs=[whole((n, 3 * HD))] * 4,
        flops=2 * n * D * 12 * HD,
        size=7 << 20,
        limit=60 << 20,
    )


def attention_body(spread, lengths, *refs):
    count = 6 * len(spread)
    qs, pieces, outs = refs[:4], refs[4 : 4 + count], refs[4 + count : 8 + count]
    q_all, k_all, v_all, o_all, peak, acc, sem = refs[8 + count :]
    c, y, x, z = seats()
    pair = lax.rem(y, 2)
    roll = lax.div(y, 2)
    length = lengths[roll]
    quarter = 2 * pair + c
    home = c == roll
    xs = [lax.rem(x + 4 + s, 4) for s in SHIFTS]
    other = 3 - y
    blocks = [y, y + 1 - 2 * pair, other, other + 1 - 2 * lax.rem(other, 2)]

    def copies(is_home, act):
        for k in range(4):
            source = lax.rem(quarter + 4 - k, 4)
            for i in range(4):
                act(pltpu.make_async_copy(qs[k].at[i], q_all.at[source * 4 + xs[i]], sem))
        for g, shifts in enumerate(spread):
            own, pa, pb, r_own, r_pa, r_pb = pieces[6 * g : 6 * g + 6]
            held = (own, pa, r_pa, r_pb) if is_home else (r_own, r_pa, pa, pb)
            for block, array in zip(blocks, held):
                for i in range(4):
                    for p, shift in enumerate(shifts):
                        at = ((block * 4 + xs[i]) * 4 + lax.rem(z + 4 + shift, 4)) * QT
                        at = pl.multiple_of(at, QT)
                        rows = pl.ds(p * QT, QT)
                        act(pltpu.make_async_copy(array.at[i, rows, pl.ds(0, HD)], k_all.at[pl.ds(at, QT), :], sem))
                        act(pltpu.make_async_copy(
                            array.at[i, rows, pl.ds(HD, HD)], v_all.at[pl.ds(at, QT), pl.ds(0, HD)], sem))

    @pl.when(home)
    def _():
        copies(True, lambda copy: copy.start())

    @pl.when(jnp.logical_not(home))
    def _():
        copies(False, lambda copy: copy.start())

    v_all[:, HD:] = jnp.ones((8192, HD), BF)
    copies(True, lambda copy: copy.wait())

    high = lax.shift_right_logical(quarter, 1)
    row_block = lax.broadcasted_iota(jnp.int32, (512, 512), 0) // QT
    key_frame = lax.broadcasted_iota(jnp.int32, (512, 512), 1) // TOK_FRAME

    def process(Y, yk, masked):
        q = q_all[pl.ds(Y * 4, 4)].reshape(512, HD)
        scores = []
        for kb in range(4):
            at = pl.multiple_of((yk * 4 + kb) * 512, 512)
            s = lax.dot_general(q, k_all[pl.ds(at, 512), :], (((1,), (1,)), ((), ())), preferred_element_type=F32)
            if masked:
                seen = 2 * (yk * 4 + kb) + key_frame
                allowed = (seen <= 2 * (4 * Y + row_block) + high) & (seen < length)
                s = jnp.where(allowed, s, -1e30)
            scores.append(s)
        top = functools.reduce(jnp.maximum, scores)
        before = peak[...]
        now = jnp.maximum(before, jnp.max(top, axis=1, keepdims=True))
        peak[...] = now
        total = acc[...] * jnp.exp2(before - now)[:, :1]
        for kb in range(4):
            at = pl.multiple_of((yk * 4 + kb) * 512, 512)
            weights = jnp.exp2(scores[kb] - now[:, :1]).astype(BF)
            total = total + jnp.dot(weights, v_all[pl.ds(at, 512), :], preferred_element_type=F32)
        acc[...] = total

    def rows_of(Y, carry):
        peak[...] = jnp.full((512, HD), -1e30, F32)
        acc[...] = jnp.zeros((512, 2 * HD), F32)
        blocks_in = lax.div(length + 7, 8)
        last = jnp.minimum(Y, blocks_in - 1)
        full = jnp.minimum(Y, lax.div(length, 8))

        def plain(yk, inner):
            process(Y, yk, False)
            return inner

        def cut(yk, inner):
            process(Y, yk, True)
            return inner

        lax.fori_loop(0, full, plain, 0)
        lax.fori_loop(full, last + 1, cut, 0)
        result = (acc[:, :HD] / acc[:, HD:]).astype(BF)
        o_all[pl.ds(Y * 4, 4)] = result.reshape(4, QT, HD)
        return carry

    lax.fori_loop(0, 4, rows_of, 0)

    def back(act):
        for k in range(4):
            source = lax.rem(quarter + 4 - k, 4)
            for i in range(4):
                act(pltpu.make_async_copy(o_all.at[source * 4 + xs[i]], outs[i].at[k], sem))

    back(lambda copy: copy.start())
    back(lambda copy: copy.wait())


def attention(lengths, qs, chunks, spread):
    pieces = [piece for chunk in chunks for piece in chunk]
    anyspace = pl.BlockSpec(memory_space=pl.ANY)
    ins = [lengths, *qs, *pieces]
    return call(
        functools.partial(attention_body, spread),
        [shape((4, QT, HD))] * 4,
        ins,
        [
            pltpu.VMEM((16, QT, HD), BF),
            pltpu.VMEM((8192, HD), BF),
            pltpu.VMEM((8192, 2 * HD), BF),
            pltpu.VMEM((16, QT, HD), BF),
            pltpu.VMEM((512, HD), F32),
            pltpu.VMEM((512, 2 * HD), F32),
            pltpu.SemaphoreType.DMA,
        ],
        in_specs=[pl.BlockSpec(memory_space=SMEM)] + [anyspace] * (len(ins) - 1),
        out_specs=[anyspace] * 4,
        flops=6 << 30,
        size=8 << 20,
        limit=48 << 20,
    )


def project_body(gain, rows, *refs):
    mixed_in, ws = refs[:4], refs[4:9]
    after, normed2, total, mixed, acc = refs[9:]
    step = pl.program_id(0)
    c, y, x, z = seats()

    @pl.when(step == 0)
    def _():
        for kk in range(4):
            z_from = lax.rem(y + 4 - kk, 4)
            for i, s in enumerate(SHIFTS):
                head = z_from * 4 + lax.rem(x + 4 - s, 4)
                mixed[:, pl.ds(pl.multiple_of(head * HD, HD), HD)] = mixed_in[kk][i]

    def term(slab, offset, w):
        at = pl.multiple_of(lax.rem(slab, 4) * 512 + offset, 256)
        return jnp.dot(mixed[:, pl.ds(at, w.shape[0])], w[...], preferred_element_type=F32)

    sums = term(z, 0, ws[0])
    sums = sums + term(z + 3 + 2 * c, 0, ws[1]) + term(z + 5 - 2 * c, 0, ws[2])
    sums = sums + term(z + 2, c * 256, ws[3]) + term(z + 2, (1 - c) * 256, ws[4])
    acc[:, pl.ds(pl.multiple_of(step * 512, 512), 512)] = sums

    @pl.when(step == 3)
    def _():
        rounded = (rows[...].astype(F32) + acc[...]).astype(BF)
        after[...] = rounded
        floats = rounded.astype(F32)
        normed2[...] = normalized(floats, gain[...])
        total[...] = jnp.broadcast_to(jnp.sum(floats, axis=0, keepdims=True), (8, D))


def project(gain, rows, mixed_in, ws):
    whole = lambda dims: pl.BlockSpec(tuple(dims), lambda n: (0,) * len(dims))
    cut = lambda w: pl.BlockSpec((w.shape[0], 512), lambda n: (0, n))
    return call(
        project_body,
        [shape((QT, D)), shape((QT, D)), shape((8, D), F32)],
        [gain, rows, *mixed_in, *ws],
        [pltpu.VMEM((QT, D), BF), pltpu.VMEM((QT, D), F32)],
        grid=(4,),
        in_specs=[whole((1, D)), whole((QT, D)), *(whole(m.shape) for m in mixed_in), *(cut(w) for w in ws)],
        out_specs=[whole((QT, D)), whole((QT, D)), whole((8, D))],
        flops=2 * QT * D * D,
        size=9 << 20,
        limit=60 << 20,
    )


def pack_body(*refs):
    out = refs[4]
    for i in range(4):
        out[i] = refs[i][...]


def pack(pieces):
    n = pieces[0].shape[0]
    return call(
        pack_body, shape((4, n, 2 * HD)), pieces, grid=(1,),
        in_specs=[pl.BlockSpec((n, 2 * HD), lambda i: (0, 0))] * 4,
        out_specs=pl.BlockSpec((4, n, 2 * HD), lambda i: (0, 0, 0)),
        flops=1 << 22, size=n << 12, limit=8 << 20,
    )


def queries_body(order, *refs):
    pieces, outs = refs[:12], refs[12:]
    c, y, x, z = seats()
    for k in range(4):
        turn = lax.rem(y + k + 4 - z, 4)
        for shift in range(4):
            group, part = order[shift]

            @pl.when(turn == shift)
            def _():
                for i in range(4):
                    outs[k][i] = pieces[group * 4 + i][part * QT : (part + 1) * QT, :]


def queries(groups, order):
    pieces = [piece for group in groups for piece in group]
    return call(
        functools.partial(queries_body, order), [shape((4, QT, HD))] * 4, pieces, grid=(1,),
        in_specs=[pl.BlockSpec((p.shape[0], HD), lambda i: (0, 2)) for p in pieces],
        out_specs=[pl.BlockSpec((4, QT, HD), lambda i: (0, 0, 0))] * 4,
        flops=1 << 22, size=1 << 20, limit=8 << 20,
    )


def heads_body(*refs):
    c, y, x, z = seats()
    quarter = 2 * lax.rem(y, 2) + c
    for kk in range(4):
        k = lax.rem(quarter + 8 - z - kk, 4)
        for i in range(4):
            refs[4 + kk][i] = refs[i][k]


def combine_body(part, to_right, to_left, left, right):
    half = QT // 2
    left[:half, :] = part[:half, :].astype(BF)
    left[half:, :] = (part[half:QT, :] + to_left[...].astype(F32)).astype(BF)
    right[:half, :] = (part[QT : QT + half, :] + to_right[...].astype(F32)).astype(BF)
    right[half:, :] = part[QT + half :, :].astype(BF)


def mlp_body(parts, *refs):
    rows, w_up, w_down, refs = refs[:parts], refs[parts], refs[parts + 1], refs[-5:]
    out, sums, inside, upper, acc = refs
    step, n = pl.program_id(0), inside.shape[0]

    @pl.when(step == 0)
    def _():
        at = 0
        for part in rows:
            inside[at : at + part.shape[0], :] = part[...]
            at += part.shape[0]
        acc[...] = jnp.zeros_like(acc)

    hidden = jnp.dot(inside[...], w_up[...], preferred_element_type=F32)
    up = jax.nn.gelu(hidden, approximate=True).astype(BF)
    upper[:n, :] = up
    index = lax.broadcasted_iota(jnp.int32, (16, up.shape[1]), 0)
    extra = jnp.zeros((16, up.shape[1]), F32)
    for q in range(n // QT):
        whole = jnp.sum(up[q * QT : (q + 1) * QT, :].astype(F32), axis=0, keepdims=True)
        high = whole.astype(BF).astype(F32)
        extra = jnp.where(index == 2 * q, high, jnp.where(index == 2 * q + 1, whole - high, extra))
    upper[n:, :] = extra.astype(BF)
    acc[...] += jnp.dot(upper[...], w_down[...], preferred_element_type=F32)

    @pl.when(step == pl.num_programs(0) - 1)
    def _():
        out[...] = acc[:n, :].astype(out.dtype)
        sums[...] = acc[n:, :]


def mlp(parts, w_up, w_down, kind, after=()):
    n = sum(part.shape[0] for part in parts)
    ff = w_up.shape[1]
    block = 512
    whole = lambda dims: pl.BlockSpec(tuple(dims), lambda f: (0,) * len(dims))
    return call(
        functools.partial(mlp_body, len(parts)),
        [shape((n, D), kind), shape((16, D), F32)],
        [*parts, w_up, w_down, *after],
        [pltpu.VMEM((n, D), BF), pltpu.VMEM((n + 16, block), BF), pltpu.VMEM((n + 16, D), F32)],
        grid=(ff // block,),
        in_specs=[*(whole(part.shape) for part in parts),
                  pl.BlockSpec((D, block), lambda f: (0, f)), pl.BlockSpec((block, D), lambda f: (f, 0)),
                  *([pl.BlockSpec(memory_space=pl.ANY)] * len(after))],
        out_specs=[whole((n, D)), whole((16, D))],
        flops=4 * n * D * ff,
        size=17 << 20,
        limit=60 << 20,
    )


def states_body(lengths, near, above, below, far, gain, bias, weight, out, means, states):
    c, y, x, z = seats()
    length = lengths[c]
    for array, ys in ((near, 0), (below, -1), (above, 1), (far, 2)):
        for i, s in enumerate(SHIFTS):
            at = lax.rem(y + 4 + ys, 4) * 4 + lax.rem(x + 4 + s, 4)
            means[at] = array[i] * (1.0 / TOK_FRAME)
    state = jnp.zeros((1, D), F32)
    for frame in range(FRAMES):
        mean = means[frame // 2, frame % 2 : frame % 2 + 1, :]
        gate = jax.nn.sigmoid(mean * gain[...] + bias[...])
        state = jnp.where(frame < length, gate * state + (1.0 - gate) * mean, state)
        states[frame : frame + 1, :] = state
    values = jnp.sum(states[...] * weight[...], axis=1, keepdims=True)
    index = lax.broadcasted_iota(jnp.int32, (FRAMES, HD), 0)
    out[...] = jnp.where(index < length, values, 0.0)


def advantages_body(lengths, mine, theirs, first, second):
    c, y, x, z = seats()
    length, length_other = lengths[c], lengths[1 - c]
    index = lax.broadcasted_iota(jnp.int32, (FRAMES, HD), 0)

    def gap_of(values, size):
        final = jnp.sum(jnp.where(index == size - 1, values, 0.0), axis=0, keepdims=True)
        return jnp.where(index < size, final - values, 0.0)

    gap, gap_other = gap_of(mine[...], length), gap_of(theirs[...], length_other)
    count = (length + length_other).astype(F32)
    summed = lambda v: jnp.sum(v, axis=0, keepdims=True)
    mean = (summed(gap) + summed(gap_other)) / count
    centered = jnp.where(index < length, gap - mean, 0.0)
    centered_other = jnp.where(index < length_other, gap_other - mean, 0.0)
    variance = (summed(centered * centered) + summed(centered_other * centered_other)) / count
    scaled = jnp.where(index < length, centered * lax.rsqrt(variance + 1e-05), 0.0)
    at = (y * 4 + x) * 2
    lane = lax.broadcasted_iota(jnp.int32, (1, HD), 1)

    def picked(values):
        one, two = (summed(jnp.where(index == at + e, values, 0.0)) for e in (0, 1))
        return jnp.where(lane == 0, one, two)[:, :2]

    first[...] = picked(mine[...])
    second[...] = picked(scaled)


def local(tokens, attn_gain, w_qkv, w_out, mlp_gain, w_up, w_down, pool_gain, pool_bias, value_weight, valid_frames):
    rows = tokens[0]
    c, y, x, z = seats()
    line = lambda v: v.reshape(1, D)

    from_left = moved(rows, "tensor", 1)
    from_right = moved(rows, "tensor", -1)
    far_top = moved(from_left[:64], "tensor", 1)
    far_low = moved(from_right[64:], "tensor", -1)
    groups = (((rows,), (0,)), ((from_left, from_right), (-1, 1)), ((far_top, far_low), (2,)))
    spread = tuple(group[1] for group in groups)

    pa_pairs, pb_pairs, to_guest, to_home = [], [], [], []
    for core in range(2):
        for yy in range(4):
            if yy // 2 == core:
                pa_pairs.append((flat(core, yy), flat(core, yy ^ 1)))
                to_guest.append((flat(core, yy), flat(1 - core, yy)))
            else:
                pa_pairs.append((flat(core, yy), flat(1 - core, 3 - yy)))
                pb_pairs.append((flat(core, yy), flat(core, yy ^ 1)))
                to_home.append((flat(core, yy), flat(1 - core, yy)))
    swap = [(0, 1), (1, 0)]

    chunks, held, order = [], [], {}
    for g, (parts, shifts) in enumerate(groups):
        made = qkv_of(line(attn_gain), parts, w_qkv)
        got = [made[0], moved(made[1], "x", 1), moved(made[3], "x", -1), moved(made[2], "x", 2)]
        held.append(got)
        block = pack(got)
        pa = lax.ppermute(block, ("dp", "y"), pa_pairs)
        pb = lax.ppermute(pa, ("dp", "y"), pb_pairs)
        r_own = lax.ppermute(block, ("dp", "y"), to_guest)
        r_pa = lax.ppermute(pa, "dp", swap)
        r_pb = lax.ppermute(pb, ("dp", "y"), to_home)
        chunks.append((block, pa, pb, r_own, r_pa, r_pb))
        for p, shift in enumerate(shifts):
            order[shift % 4] = (g, p)
    qs = []
    for k, part in enumerate(queries(held, order)):
        pairs = []
        for core in range(2):
            for yy in range(4):
                j = (yy + k) % 4
                pairs.append((flat(core, yy), flat(j % 2, 2 * core + j // 2)))
        qs.append(lax.ppermute(part, ("dp", "y"), pairs))

    outs = attention(valid_frames, qs, chunks, spread)

    w_first, _ = lax.optimization_barrier((w_out, far_low))
    pairs = [(4 * core + zz, 4 * core + (zz + 1 - 2 * core) % 4) for core in range(2) for zz in range(4)]
    w_near = lax.ppermute(w_first, ("dp", "tensor"), pairs)
    w_far = lax.ppermute(lax.dynamic_slice(w_near, (c * 256, 0), (256, D)), ("dp", "tensor"), pairs)
    ws = [w_out, w_near, lax.ppermute(w_near, "dp", swap), w_far, lax.ppermute(w_far, "dp", swap)]

    heads = [outs[0], moved(outs[1], "x", -1), moved(outs[2], "x", 1), moved(outs[3], "x", 2)]
    mixed_in = []
    for kk, part in enumerate(call(heads_body, [shape((4, QT, HD))] * 4, heads, flops=1 << 22, size=1 << 20, limit=8 << 20)):
        pairs = []
        for core in range(2):
            for yy in range(4):
                for zz in range(4):
                    j = 2 * (yy % 2) + core
                    pairs.append((flat(core, yy, zz), flat(yy // 2, (zz + kk) % 4, j)))
        mixed_in.append(lax.ppermute(part, ("dp", "y", "tensor"), pairs))
    after, normed2, after_sum = project(line(mlp_gain), rows, mixed_in, ws)

    top, low = normed2[:64], normed2[64:]
    left_top = moved(top, "tensor", 1)
    right_low = moved(low, "tensor", -1)
    opposite_top = moved(left_top, "tensor", 1)
    opposite_low = moved(right_low, "tensor", -1)
    top, low, _, _ = lax.optimization_barrier((top, low, left_top, right_low))
    left_low = moved(low, "tensor", 1)
    right_top = moved(top, "tensor", -1)
    far_part, far_sums = mlp((opposite_top, opposite_low), w_up, w_down, BF)
    near_part, near_sums = mlp((left_top, left_low, right_top, right_low, normed2), w_up, w_down, F32, (far_sums,))
    to_right = moved(far_part[:64], "tensor", 1)
    to_left = moved(far_part[64:], "tensor", -1)
    for_left, for_right = call(
        combine_body, [shape((QT, D))] * 2, [near_part, to_right, to_left], grid=(1,),
        in_specs=[pl.BlockSpec((2 * QT, D), lambda i: (0, 0)), *([pl.BlockSpec((QT // 2, D), lambda i: (0, 0))] * 2)],
        out_specs=[pl.BlockSpec((QT, D), lambda i: (0, 0))] * 2, flops=1 << 22, size=4 << 20, limit=16 << 20,
    )
    sum_one = moved(for_right, "tensor", 1)
    sum_two = moved(for_left, "tensor", -1)
    hidden = (after.astype(F32) + near_part[2 * QT :] + sum_one.astype(F32) + sum_two.astype(F32)).astype(BF)

    own_total = near_sums[4] + near_sums[5] + after_sum[0]
    far_total = far_sums[0] + far_sums[1]
    left_total = near_sums[0] + near_sums[1]
    right_total = near_sums[2] + near_sums[3]
    totals = jnp.zeros((2, D), F32)
    for shift, part in ((0, own_total), (-1, left_total), (1, right_total), (2, far_total)):
        frame = ((z + shift) % 4) // 2
        totals = totals + jnp.where(jnp.arange(2)[:, None] == frame, part[None], 0.0)
    totals = totals + moved(totals, "tensor", 1) + moved(totals, "tensor", -1) + moved(totals, "tensor", 2)
    over_x = jnp.stack([totals, moved(totals, "x", 1), moved(totals, "x", -1), moved(totals, "x", 2)])
    below, above, across = moved(over_x, "y", 1), moved(over_x, "y", -1), moved(over_x, "y", 2)
    values = call(
        states_body,
        shape((FRAMES, HD), F32),
        [valid_frames, over_x, above, below, across, line(pool_gain), line(pool_bias), line(value_weight)],
        [pltpu.VMEM((16, 2, D), F32), pltpu.VMEM((FRAMES, D), F32)],
        in_specs=[pl.BlockSpec(memory_space=SMEM)] + [pl.BlockSpec(memory_space=VMEM)] * 7,
        flops=1 << 20,
        size=1 << 20,
        limit=8 << 20,
    )
    other_values = lax.ppermute(values, "dp", swap)
    frame_values, advantages = call(
        advantages_body,
        [shape((1, 2), F32)] * 2,
        [valid_frames, values, other_values],
        in_specs=[pl.BlockSpec(memory_space=SMEM)] + [pl.BlockSpec(memory_space=VMEM)] * 2,
        flops=1 << 14,
        size=1 << 15,
        limit=4 << 20,
    )
    return hidden[None], frame_values, advantages


def solution(mesh):
    fine = Mesh(mesh.devices.reshape(2, 4, 4, 4), ("dp", "y", "x", "tensor"))
    token_spec = P("dp", ("y", "x", "tensor"), None)
    in_specs = (
        token_spec,
        P(),
        P(None, None, "tensor"),
        P("tensor", None),
        P(),
        P(None, "tensor"),
        P("tensor", None),
        P(),
        P(),
        P(),
        P(),
    )
    out_specs = (token_spec, P("dp", ("y", "x")), P("dp", ("y", "x")))
    return jax.shard_map(local, mesh=fine, in_specs=in_specs, out_specs=out_specs, check_vma=False)
```

```python
import functools
import math

import jax
import jax.numpy as jnp
from jax import lax
from jax.experimental import pallas as pl
from jax.experimental.pallas import tpu as pltpu
from jax.sharding import Mesh, PartitionSpec as P


D = 2048
HD = 128
QT = 128
FRAMES = 32
TOK_FRAME = 256
BF = jnp.bfloat16
F32 = jnp.float32
QSCALE = math.log2(math.e) / math.sqrt(HD)
SHIFTS = (0, -1, 1, 2)
VMEM = pltpu.VMEM
SMEM = pltpu.SMEM


def ring(shift):
    return [(i, (i + shift) % 4) for i in range(4)]


def moved(array, axis, shift):
    return lax.ppermute(array, axis, ring(shift))


def flat(*digits):
    sizes = {2: (2, 4), 3: (2, 4, 4)}[len(digits)]
    at = 0
    for digit, size in zip(digits, sizes):
        at = at * size + digit
    return at


def seats():
    return tuple(lax.axis_index(name).astype(jnp.int32) for name in ("dp", "y", "x", "tensor"))


def call(body, out, ins, scratch=(), grid=None, in_specs=None, out_specs=None, flops=0, size=0, limit=None):
    single = not isinstance(out, (list, tuple))
    outs = [out] if single else list(out)
    whole = pl.BlockSpec(memory_space=VMEM)
    kwargs = {} if grid is None else {"grid": grid}
    return pl.pallas_call(
        body,
        out_shape=out if single else outs,
        in_specs=in_specs or [whole] * len(ins),
        out_specs=out_specs or (whole if single else [whole] * len(outs)),
        scratch_shapes=list(scratch),
        compiler_params=pltpu.CompilerParams(vmem_limit_bytes=limit),
        cost_estimate=pl.CostEstimate(flops=flops, bytes_accessed=size, transcendentals=0),
        **kwargs,
    )(*ins)


def shape(dims, kind=BF):
    return jax.ShapeDtypeStruct(tuple(dims), kind)


def normalized(floats, gain):
    square = jnp.mean(floats * floats, axis=-1, keepdims=True)
    return (floats * lax.rsqrt(square + 1e-05) * gain).astype(BF)


def qkv_body(parts, gain, *refs):
    place = seats()
    rows, w, outs, normed, made = refs[:parts], refs[parts], refs[parts + 1 : parts + 5], refs[-2], refs[-1]
    step = pl.program_id(0)

    @pl.when(step == 0)
    def _():
        at = 0
        for part in rows:
            n = part.shape[0]
            normed[at : at + n, :] = normalized(part[...].astype(F32), gain[...])
            at += n

    product = jnp.dot(normed[...], w[0], preferred_element_type=F32)
    product = product * jnp.where(step == 0, QSCALE, 1.0)
    made[...] = product.astype(BF)
    slot = lax.rem(step + 2, 3)
    for rel in range(4):
        head = lax.rem(place[2] + rel, 4)
        outs[rel][:, pl.ds(pl.multiple_of(slot * HD, HD), HD)] = made[:, pl.ds(pl.multiple_of(head * HD, HD), HD)]


def qkv_of(gain, parts, w):
    n = sum(part.shape[0] for part in parts)
    whole = lambda dims: pl.BlockSpec(tuple(dims), lambda c: (0,) * len(dims))
    return call(
        functools.partial(qkv_body, len(parts)),
        [shape((n, 3 * HD))] * 4,
        [gain, *parts, w],
        [pltpu.VMEM((n, D), BF), pltpu.VMEM((n, 4 * HD), BF)],
        grid=(3,),
        in_specs=[whole((1, D)), *(whole(part.shape) for part in parts),
                  pl.BlockSpec((1, D, 4 * HD), lambda c: (c, 0, 0))],
        out_specs=[whole((n, 3 * HD))] * 4,
        flops=2 * n * D * 12 * HD,
        size=7 << 20,
        limit=24 << 20,
    )


def attention_body(spread, lengths, *refs):
    qs, mine, theirs, outs = refs[:4], refs[4], refs[5], refs[6:10]
    q_all, k_all, v_all, o_all, held, peak, acc, sem = refs[10:]
    c, y, x, z = seats()
    pair = lax.rem(y, 2)
    roll = lax.div(y, 2)
    length = lengths[roll]
    quarter = 2 * pair + c
    home = c == roll
    xs = [lax.rem(x + 4 + s, 4) for s in SHIFTS]
    twin = lambda v: v + 1 - 2 * lax.rem(v, 2)
    first, second = jnp.where(home, y, 3 - y), jnp.where(home, 3 - y, y)
    blocks = ((mine, 0, first), (mine, 1, twin(first)), (theirs, 0, second), (theirs, 1, twin(second)))

    def copies(act):
        for k in range(4):
            source = lax.rem(quarter + 4 - k, 4)
            for i in range(4):
                act(pltpu.make_async_copy(qs[k].at[i], q_all.at[source * 4 + xs[i]], sem))
        for array, b, block in blocks:
            for i in range(4):
                for p, shift in enumerate(spread):
                    at = ((block * 4 + xs[i]) * 4 + lax.rem(z + 4 + shift, 4)) * QT
                    at = pl.ds(pl.multiple_of(at, QT), QT)
                    rows = pl.ds(p * QT, QT)
                    act(pltpu.make_async_copy(array.at[b, i, rows, pl.ds(0, HD)], k_all.at[at, :], sem))
                    act(pltpu.make_async_copy(array.at[b, i, rows, pl.ds(HD, HD)], v_all.at[at, pl.ds(0, HD)], sem))

    copies(lambda copy: copy.start())
    v_all[:, HD:] = jnp.ones((8192, HD), BF)
    copies(lambda copy: copy.wait())

    high = lax.shift_right_logical(quarter, 1)
    blocks_in = lax.div(length + 7, 8)
    parts = [slice(rb * QT, (rb + 1) * QT) for rb in range(4)]

    def bias(Y, yk, kb, rb, half):
        seen = 2 * (yk * 4 + kb) + half
        return jnp.where((seen <= 2 * (4 * Y + rb) + high) & (seen < length), 0.0, -1e30).astype(F32)

    def keys_at(yk, kb):
        return pl.ds(pl.multiple_of((yk * 4 + kb) * 512, 512), 512)

    def score(Y, yk, kb, tops):
        q = q_all[pl.ds(Y * 4, 4)].reshape(512, HD)
        s = lax.dot_general(q, k_all[keys_at(yk, kb), :], (((1,), (1,)), ((), ())), preferred_element_type=F32)
        held[kb] = s
        made = []
        for rb in range(4):
            top = tops[rb]
            for half in range(2):
                piece = s[parts[rb], half * TOK_FRAME : (half + 1) * TOK_FRAME]
                top = jnp.maximum(top, jnp.maximum(piece[:, :HD], piece[:, HD:]) + bias(Y, yk, kb, rb, half))
            made.append(top)
        return made

    def row_top(top):
        return jnp.max(top, axis=1, keepdims=True)

    def start_rows(tops):
        acc[...] = jnp.zeros((512, 2 * HD), F32)
        for rb in range(4):
            peak[parts[rb], :] = jnp.broadcast_to(row_top(tops[rb]), (QT, HD))

    lowest = [jnp.full((QT, HD), -1e30, F32)] * 4
    tops = lowest
    for kb in range(4):
        tops = score(0, 0, kb, tops)
    start_rows(tops)

    def step(_, at):
        Y, yk = at
        last = yk >= jnp.minimum(Y, blocks_in - 1)
        next_Y, next_k = jnp.where(last, Y + 1, Y), jnp.where(last, 0, yk + 1)
        inside_Y = jnp.minimum(next_Y, 3)
        tops, total = lowest, acc[...]
        m = [peak[part, :1] for part in parts]
        for kb in range(4):
            rows = []
            for rb in range(4):
                row = [
                    jnp.exp2(held[kb, parts[rb], half * TOK_FRAME : (half + 1) * TOK_FRAME]
                             - (m[rb] - bias(Y, yk, kb, rb, half))).astype(BF)
                    for half in range(2)
                ]
                rows.append(jnp.concatenate(row, axis=1))
            weights = jnp.concatenate(rows, axis=0)
            total = total + jnp.dot(weights, v_all[keys_at(yk, kb), :], preferred_element_type=F32)
            tops = score(inside_Y, next_k, kb, tops)

        @pl.when(last)
        def _():
            o_all[pl.ds(Y * 4, 4)] = (total[:, :HD] / total[:, HD:]).astype(BF).reshape(4, QT, HD)
            start_rows(tops)

        @pl.when(jnp.logical_not(last))
        def _():
            for rb in range(4):
                now = jnp.maximum(m[rb], row_top(tops[rb]))
                acc[parts[rb], :] = total[parts[rb]] * jnp.exp2(m[rb] - now)
                peak[parts[rb], :] = jnp.broadcast_to(now, (QT, HD))

        return next_Y, next_k

    steps = sum(jnp.minimum(Y + 1, blocks_in) for Y in range(4))
    lax.fori_loop(0, steps, step, (jnp.int32(0), jnp.int32(0)))

    def back(act):
        for k in range(4):
            source = lax.rem(quarter + 4 - k, 4)
            for i in range(4):
                act(pltpu.make_async_copy(o_all.at[source * 4 + xs[i]], outs[i].at[k], sem))

    back(lambda copy: copy.start())
    back(lambda copy: copy.wait())


def attention(lengths, qs, mine, theirs, spread):
    anyspace = pl.BlockSpec(memory_space=pl.ANY)
    ins = [lengths, *qs, mine, theirs]
    return call(
        functools.partial(attention_body, spread),
        [shape((4, QT, HD))] * 4,
        ins,
        [
            pltpu.VMEM((16, QT, HD), BF),
            pltpu.VMEM((8192, HD), BF),
            pltpu.VMEM((8192, 2 * HD), BF),
            pltpu.VMEM((16, QT, HD), BF),
            pltpu.VMEM((4, 512, 512), F32),
            pltpu.VMEM((512, HD), F32),
            pltpu.VMEM((512, 2 * HD), F32),
            pltpu.SemaphoreType.DMA,
        ],
        in_specs=[pl.BlockSpec(memory_space=SMEM)] + [anyspace] * (len(ins) - 1),
        out_specs=[anyspace] * 4,
        flops=6 << 30,
        size=8 << 20,
        limit=28 << 20,
    )


def project_body(gain, rows, *refs):
    mixed_in, ws = refs[:4], refs[4:9]
    after, top, low, total, mixed, acc = refs[9:]
    step = pl.program_id(0)
    c, y, x, z = seats()

    @pl.when(step == 0)
    def _():
        for kk in range(4):
            z_from = lax.rem(y + 4 - kk, 4)
            for i, s in enumerate(SHIFTS):
                head = z_from * 4 + lax.rem(x + 4 - s, 4)
                mixed[:, pl.ds(pl.multiple_of(head * HD, HD), HD)] = mixed_in[kk][i]

    def term(slab, offset, w):
        at = pl.multiple_of(lax.rem(slab, 4) * 512 + offset, 256)
        return jnp.dot(mixed[:, pl.ds(at, w.shape[0])], w[...], preferred_element_type=F32)

    sums = term(z, 0, ws[0])
    sums = sums + term(z + 3 + 2 * c, 0, ws[1]) + term(z + 5 - 2 * c, 0, ws[2])
    sums = sums + term(z + 2, c * 256, ws[3]) + term(z + 2, (1 - c) * 256, ws[4])
    acc[:, pl.ds(pl.multiple_of(step * 512, 512), 512)] = sums

    @pl.when(step == 3)
    def _():
        rounded = (rows[...].astype(F32) + acc[...]).astype(BF)
        after[...] = rounded
        floats = rounded.astype(F32)
        normed2 = normalized(floats, gain[...])
        top[...] = normed2[: QT // 2]
        low[...] = normed2[QT // 2 :]
        total[...] = jnp.broadcast_to(jnp.sum(floats, axis=0, keepdims=True), (8, D))


def project(gain, rows, mixed_in, ws):
    whole = lambda dims: pl.BlockSpec(tuple(dims), lambda n: (0,) * len(dims))
    cut = lambda w: pl.BlockSpec((w.shape[0], 512), lambda n: (0, n))
    return call(
        project_body,
        [shape((QT, D)), shape((QT // 2, D)), shape((QT // 2, D)), shape((8, D), F32)],
        [gain, rows, *mixed_in, *ws],
        [pltpu.VMEM((QT, D), BF), pltpu.VMEM((QT, D), F32)],
        grid=(4,),
        in_specs=[whole((1, D)), whole((QT, D)), *(whole(m.shape) for m in mixed_in), *(cut(w) for w in ws)],
        out_specs=[whole((QT, D)), whole((QT // 2, D)), whole((QT // 2, D)), whole((8, D))],
        flops=2 * QT * D * D,
        size=9 << 20,
        limit=20 << 20,
    )


def pack_body(*refs):
    out = refs[4]
    for i in range(4):
        out[i] = refs[i][...]


def pack(pieces):
    n = pieces[0].shape[0]
    return call(
        pack_body, shape((4, n, 2 * HD)), pieces, grid=(1,),
        in_specs=[pl.BlockSpec((n, 2 * HD), lambda i: (0, 0))] * 4,
        out_specs=pl.BlockSpec((4, n, 2 * HD), lambda i: (0, 0, 0)),
        flops=1 << 22, size=n << 12, limit=8 << 20,
    )


def share_body(*refs):
    out = refs[9]
    c, y, _, _ = seats()
    for pick, when in ((0, c == lax.div(y, 2)), (1, c != lax.div(y, 2))):

        @pl.when(when)
        def _():
            for b in range(2):
                at = 0
                for g in range(3):
                    part = refs[3 * g + pick + b]
                    out[b, :, at : at + part.shape[1], :] = part[...]
                    at += part.shape[1]


def queries_body(order, *refs):
    pieces, outs = refs[:12], refs[12:]
    _, y, _, z = seats()
    for k in range(4):
        turn = lax.rem(y + k + 4 - z, 4)
        for shift in range(4):
            group, part = order[shift]

            @pl.when(turn == shift)
            def _():
                for i in range(4):
                    outs[k][i] = pieces[group * 4 + i][part * QT : (part + 1) * QT, :]


def queries(groups, order):
    pieces = [piece for group in groups for piece in group]
    return call(
        functools.partial(queries_body, order), [shape((4, QT, HD))] * 4, pieces, grid=(1,),
        in_specs=[pl.BlockSpec((p.shape[0], HD), lambda i: (0, 2)) for p in pieces],
        out_specs=[pl.BlockSpec((4, QT, HD), lambda i: (0, 0, 0))] * 4,
        flops=1 << 22, size=1 << 20, limit=8 << 20,
    )


def heads_body(*refs):
    c, y, _, z = seats()
    quarter = 2 * lax.rem(y, 2) + c
    for kk in range(4):
        k = lax.rem(quarter + 8 - z - kk, 4)
        for i in range(4):
            refs[4 + kk][i] = refs[i][k]


def combine_body(part, to_right, to_left, left, right):
    half = QT // 2
    left[:half, :] = part[:half, :].astype(BF)
    left[half:, :] = (part[half:QT, :] + to_left[...].astype(F32)).astype(BF)
    right[:half, :] = (part[QT : QT + half, :] + to_right[...].astype(F32)).astype(BF)
    right[half:, :] = part[QT + half :, :].astype(BF)


def mlp_body(parts, cuts, *refs):
    rows, w_up, w_down = refs[:parts], refs[parts], refs[parts + 1]
    outs = refs[-4 - len(cuts) : -4]
    sums, inside, upper, acc = refs[-4:]
    step, n = pl.program_id(0), inside.shape[0]

    @pl.when(step == 0)
    def _():
        at = 0
        for part in rows:
            inside[at : at + part.shape[0], :] = part[...]
            at += part.shape[0]
        acc[...] = jnp.zeros_like(acc)

    hidden = jnp.dot(inside[...], w_up[...], preferred_element_type=F32)
    up = jax.nn.gelu(hidden, approximate=True).astype(BF)
    upper[:n, :] = up
    index = lax.broadcasted_iota(jnp.int32, (16, up.shape[1]), 0)
    extra = jnp.zeros((16, up.shape[1]), F32)
    for q in range(n // QT):
        whole = jnp.sum(up[q * QT : (q + 1) * QT, :].astype(F32), axis=0, keepdims=True)
        high = whole.astype(BF).astype(F32)
        extra = jnp.where(index == 2 * q, high, jnp.where(index == 2 * q + 1, whole - high, extra))
    upper[n:, :] = extra.astype(BF)
    acc[...] += jnp.dot(upper[...], w_down[...], preferred_element_type=F32)

    @pl.when(step == pl.num_programs(0) - 1)
    def _():
        at = 0
        for out in outs:
            out[...] = acc[at : at + out.shape[0], :].astype(out.dtype)
            at += out.shape[0]
        sums[...] = acc[n:, :]


def mlp(parts, w_up, w_down, cuts, after=()):
    n = sum(part.shape[0] for part in parts)
    ff = w_up.shape[1]
    block = 512
    whole = lambda dims: pl.BlockSpec(tuple(dims), lambda f: (0,) * len(dims))
    return call(
        functools.partial(mlp_body, len(parts), cuts),
        [*(shape((size, D), kind) for size, kind in cuts), shape((16, D), F32)],
        [*parts, w_up, w_down, *after],
        [pltpu.VMEM((n, D), BF), pltpu.VMEM((n + 16, block), BF), pltpu.VMEM((n + 16, D), F32)],
        grid=(ff // block,),
        in_specs=[*(whole(part.shape) for part in parts),
                  pl.BlockSpec((D, block), lambda f: (0, f)), pl.BlockSpec((block, D), lambda f: (f, 0)),
                  *([pl.BlockSpec(memory_space=pl.ANY)] * len(after))],
        out_specs=[*(whole((size, D)) for size, _ in cuts), whole((16, D))],
        flops=4 * n * D * ff,
        size=17 << 20,
        limit=28 << 20,
    )


def half_body(w, out, sem):
    rows = pl.ds(pl.multiple_of(lax.axis_index("dp").astype(jnp.int32) * 256, 256), 256)
    copy = pltpu.make_async_copy(w.at[rows, :], out, sem)
    copy.start()
    copy.wait()


def totals_body(near, far, after, out):
    z = seats()[3]
    own = near[4:5, :] + near[5:6, :] + after[0:1, :]
    parts = ((0, own), (3, near[0:1, :] + near[1:2, :]), (1, near[2:3, :] + near[3:4, :]), (2, far[0:1, :] + far[1:2, :]))
    for frame in range(2):
        total = jnp.zeros((1, D), F32)
        for shift, part in parts:
            total = total + part * jnp.where(lax.rem(z + shift, 4) // 2 == frame, 1.0, 0.0)
        out[frame : frame + 1, :] = total


def stack_body(*refs):
    for i in range(4):
        refs[4][i] = refs[i][...]


def sum_body(*refs):
    refs[4][...] = refs[0][...] + refs[1][...] + refs[2][...] + refs[3][...]


def states_body(lengths, near, above, below, far, gain, bias, weight, out, means, states):
    c, y, x, _ = seats()
    length = lengths[c]
    for array, ys in ((near, 0), (below, -1), (above, 1), (far, 2)):
        for i, s in enumerate(SHIFTS):
            at = lax.rem(y + 4 + ys, 4) * 4 + lax.rem(x + 4 + s, 4)
            means[at] = array[i] * (1.0 / TOK_FRAME)
    state = jnp.zeros((1, D), F32)
    for frame in range(FRAMES):
        mean = means[frame // 2, frame % 2 : frame % 2 + 1, :]
        gate = jax.nn.sigmoid(mean * gain[...] + bias[...])
        state = jnp.where(frame < length, gate * state + (1.0 - gate) * mean, state)
        states[frame : frame + 1, :] = state
    values = jnp.sum(states[...] * weight[...], axis=1, keepdims=True)
    index = lax.broadcasted_iota(jnp.int32, (FRAMES, HD), 0)
    out[...] = jnp.where(index < length, values, 0.0)


def advantages_body(lengths, mine, theirs, first, second):
    c, y, x, _ = seats()
    length, length_other = lengths[c], lengths[1 - c]
    index = lax.broadcasted_iota(jnp.int32, (FRAMES, HD), 0)

    def gap_of(values, size):
        final = jnp.sum(jnp.where(index == size - 1, values, 0.0), axis=0, keepdims=True)
        return jnp.where(index < size, final - values, 0.0)

    gap, gap_other = gap_of(mine[...], length), gap_of(theirs[...], length_other)
    count = (length + length_other).astype(F32)
    summed = lambda v: jnp.sum(v, axis=0, keepdims=True)
    mean = (summed(gap) + summed(gap_other)) / count
    centered = jnp.where(index < length, gap - mean, 0.0)
    centered_other = jnp.where(index < length_other, gap_other - mean, 0.0)
    variance = (summed(centered * centered) + summed(centered_other * centered_other)) / count
    scaled = jnp.where(index < length, centered * lax.rsqrt(variance + 1e-05), 0.0)
    at = (y * 4 + x) * 2
    lane = lax.broadcasted_iota(jnp.int32, (1, HD), 1)

    def picked(values):
        one, two = (summed(jnp.where(index == at + e, values, 0.0)) for e in (0, 1))
        return jnp.where(lane == 0, one, two)[:, :2]

    first[...] = picked(mine[...])
    second[...] = picked(scaled)


def local(tokens, attn_gain, w_qkv, w_out, mlp_gain, w_up, w_down, pool_gain, pool_bias, value_weight, valid_frames):
    rows = tokens[0]
    line = lambda v: v.reshape(1, D)

    from_left = moved(rows, "tensor", 1)
    from_right = moved(rows, "tensor", -1)
    far_top = moved(from_left[:64], "tensor", 1)
    far_low = moved(from_right[64:], "tensor", -1)
    groups = (((rows,), (0,)), ((from_left, from_right), (-1, 1)), ((far_top, far_low), (2,)))
    spread = tuple(shift for group in groups for shift in group[1])

    pa_pairs, pb_pairs = [], []
    for core in range(2):
        for yy in range(4):
            if yy // 2 == core:
                pa_pairs.append((flat(core, yy), flat(core, yy ^ 1)))
            else:
                pa_pairs.append((flat(core, yy), flat(1 - core, 3 - yy)))
                pb_pairs.append((flat(core, yy), flat(core, yy ^ 1)))
    swap = [(0, 1), (1, 0)]

    chunks, held, order = [], [], {}
    for g, (parts, shifts) in enumerate(groups):
        made = qkv_of(line(attn_gain), parts, w_qkv)
        got = [made[0], moved(made[1], "x", 1), moved(made[3], "x", -1), moved(made[2], "x", 2)]
        held.append(got)
        block = pack(got)
        pa = lax.ppermute(block, ("dp", "y"), pa_pairs)
        pb = lax.ppermute(pa, ("dp", "y"), pb_pairs)
        chunks.extend((block, pa, pb))
        for p, shift in enumerate(shifts):
            order[shift % 4] = (g, p)
    qs = []
    for k, part in enumerate(queries(held, order)):
        pairs = []
        for core in range(2):
            for yy in range(4):
                j = (yy + k) % 4
                pairs.append((flat(core, yy), flat(j % 2, 2 * core + j // 2)))
        qs.append(lax.ppermute(part, ("dp", "y"), pairs))

    mine = call(share_body, shape((2, 4, 512, 2 * HD)), chunks, flops=1 << 24, size=4 << 20, limit=16 << 20)
    theirs = lax.ppermute(mine, "dp", swap)

    w_first, _, _ = lax.optimization_barrier((w_out, far_low, far_top))
    pairs = [(4 * core + zz, 4 * core + (zz + 1 - 2 * core) % 4) for core in range(2) for zz in range(4)]
    w_near = lax.ppermute(w_first, ("dp", "tensor"), pairs)
    w_half = call(
        half_body, shape((256, D)), [w_near], [pltpu.SemaphoreType.DMA],
        in_specs=[pl.BlockSpec(memory_space=pl.ANY)], flops=1 << 22, size=2 << 20, limit=4 << 20,
    )
    w_far = lax.ppermute(w_half, ("dp", "tensor"), pairs)
    ws = [w_out, w_near, lax.ppermute(w_near, "dp", swap), w_far, lax.ppermute(w_far, "dp", swap)]

    outs = attention(valid_frames, qs, mine, theirs, spread)

    heads = [outs[0], moved(outs[1], "x", -1), moved(outs[2], "x", 1), moved(outs[3], "x", 2)]
    heads = call(heads_body, [shape((4, QT, HD))] * 4, heads, flops=1 << 22, size=1 << 20, limit=8 << 20)
    mixed_in = []
    for kk, part in enumerate(heads):
        pairs = []
        for core in range(2):
            for yy in range(4):
                for zz in range(4):
                    j = 2 * (yy % 2) + core
                    pairs.append((flat(core, yy, zz), flat(yy // 2, (zz + kk) % 4, j)))
        mixed_in.append(lax.ppermute(part, ("dp", "y", "tensor"), pairs))
    after, top, low, after_sum = project(line(mlp_gain), rows, mixed_in, ws)

    left_top = moved(top, "tensor", 1)
    right_low = moved(low, "tensor", -1)
    opposite_top = moved(left_top, "tensor", 1)
    opposite_low = moved(right_low, "tensor", -1)
    left_low = moved(low, "tensor", 1)
    right_top = moved(top, "tensor", -1)
    far_upper, far_lower, far_sums = mlp((opposite_top, opposite_low), w_up, w_down, ((64, BF), (64, BF)))
    near_in = (left_top, left_low, right_top, right_low, top, low)
    side_part, own_part, near_sums = mlp(near_in, w_up, w_down, ((256, F32), (128, F32)), (far_sums,))
    to_right = moved(far_upper, "tensor", 1)
    to_left = moved(far_lower, "tensor", -1)
    for_left, for_right = call(
        combine_body, [shape((QT, D))] * 2, [side_part, to_right, to_left], grid=(1,),
        in_specs=[pl.BlockSpec((2 * QT, D), lambda i: (0, 0)), *([pl.BlockSpec((QT // 2, D), lambda i: (0, 0))] * 2)],
        out_specs=[pl.BlockSpec((QT, D), lambda i: (0, 0))] * 2, flops=1 << 22, size=4 << 20, limit=16 << 20,
    )
    sum_one = moved(for_right, "tensor", 1)
    sum_two = moved(for_left, "tensor", -1)
    hidden = (after.astype(F32) + own_part + sum_one.astype(F32) + sum_two.astype(F32)).astype(BF)

    totals = call(
        totals_body, shape((2, D), F32), [near_sums, far_sums, after_sum], flops=1 << 16, size=1 << 19, limit=4 << 20,
    )
    rest = [moved(totals, "tensor", s) for s in (1, -1, 2)]
    totals = call(sum_body, shape((2, D), F32), [totals, *rest], flops=1 << 14, size=1 << 17, limit=4 << 20)
    rest = [moved(totals, "x", s) for s in (1, -1, 2)]
    over_x = call(stack_body, shape((4, 2, D), F32), [totals, *rest], flops=1 << 14, size=1 << 17, limit=4 << 20)
    below, above, across = (moved(over_x, "y", s) for s in (1, -1, 2))
    values = call(
        states_body,
        shape((FRAMES, HD), F32),
        [valid_frames, over_x, above, below, across, line(pool_gain), line(pool_bias), line(value_weight)],
        [pltpu.VMEM((16, 2, D), F32), pltpu.VMEM((FRAMES, D), F32)],
        in_specs=[pl.BlockSpec(memory_space=SMEM)] + [pl.BlockSpec(memory_space=VMEM)] * 7,
        flops=1 << 20,
        size=1 << 20,
        limit=8 << 20,
    )
    other_values = lax.ppermute(values, "dp", swap)
    frame_values, advantages = call(
        advantages_body,
        [shape((1, 2), F32)] * 2,
        [valid_frames, values, other_values],
        in_specs=[pl.BlockSpec(memory_space=SMEM)] + [pl.BlockSpec(memory_space=VMEM)] * 2,
        flops=1 << 14,
        size=1 << 15,
        limit=4 << 20,
    )
    return hidden[None], frame_values, advantages


def solution(mesh):
    fine = Mesh(mesh.devices.reshape(2, 4, 4, 4), ("dp", "y", "x", "tensor"))
    token_spec = P("dp", ("y", "x", "tensor"), None)
    in_specs = (
        token_spec,
        P(),
        P(None, None, "tensor"),
        P("tensor", None),
        P(),
        P(None, "tensor"),
        P("tensor", None),
        P(),
        P(),
        P(),
        P(),
    )
    out_specs = (token_spec, P("dp", ("y", "x")), P("dp", ("y", "x")))
    return jax.shard_map(local, mesh=fine, in_specs=in_specs, out_specs=out_specs, check_vma=False)
```

```python
import functools
import math

import jax
import jax.numpy as jnp
from jax import lax
from jax.experimental import pallas as pl
from jax.experimental.pallas import tpu as pltpu
from jax.sharding import Mesh, PartitionSpec as P


D = 2048
HD = 128
QT = 128
FRAMES = 32
TOK_FRAME = 256
BF = jnp.bfloat16
F32 = jnp.float32
QSCALE = math.log2(math.e) / math.sqrt(HD)
SHIFTS = (0, -1, 1, 2)
VMEM = pltpu.VMEM
SMEM = pltpu.SMEM


def ring(shift):
    return [(i, (i + shift) % 4) for i in range(4)]


def moved(array, axis, shift):
    return lax.ppermute(array, axis, ring(shift))


def flat(*digits):
    sizes = {2: (2, 4), 3: (2, 4, 4)}[len(digits)]
    at = 0
    for digit, size in zip(digits, sizes):
        at = at * size + digit
    return at


def seats():
    return tuple(lax.axis_index(name).astype(jnp.int32) for name in ("dp", "y", "x", "tensor"))


def call(body, out, ins, scratch=(), grid=None, in_specs=None, out_specs=None, flops=0, size=0, limit=None):
    single = not isinstance(out, (list, tuple))
    outs = [out] if single else list(out)
    whole = pl.BlockSpec(memory_space=VMEM)
    kwargs = {} if grid is None else {"grid": grid}
    return pl.pallas_call(
        body,
        out_shape=out if single else outs,
        in_specs=in_specs or [whole] * len(ins),
        out_specs=out_specs or (whole if single else [whole] * len(outs)),
        scratch_shapes=list(scratch),
        compiler_params=pltpu.CompilerParams(vmem_limit_bytes=limit),
        cost_estimate=pl.CostEstimate(flops=flops, bytes_accessed=size, transcendentals=0),
        **kwargs,
    )(*ins)


def shape(dims, kind=BF):
    return jax.ShapeDtypeStruct(tuple(dims), kind)


def normalized(floats, gain):
    square = jnp.mean(floats * floats, axis=-1, keepdims=True)
    return (floats * lax.rsqrt(square + 1e-05) * gain).astype(BF)


def qkv_body(parts, gain, *refs):
    place = seats()
    rows, w, outs, normed, made = refs[:parts], refs[parts], refs[parts + 1 : parts + 5], refs[-2], refs[-1]
    step = pl.program_id(0)

    @pl.when(step == 0)
    def _():
        at = 0
        for part in rows:
            n = part.shape[0]
            normed[at : at + n, :] = normalized(part[...].astype(F32), gain[...])
            at += n

    product = jnp.dot(normed[...], w[0], preferred_element_type=F32)
    product = product * jnp.where(step == 0, QSCALE, 1.0)
    made[...] = product.astype(BF)
    slot = lax.rem(step + 2, 3)
    for rel in range(4):
        head = lax.rem(place[2] + rel, 4)
        outs[rel][:, pl.ds(pl.multiple_of(slot * HD, HD), HD)] = made[:, pl.ds(pl.multiple_of(head * HD, HD), HD)]


def qkv_of(gain, parts, w):
    n = sum(part.shape[0] for part in parts)
    whole = lambda dims: pl.BlockSpec(tuple(dims), lambda c: (0,) * len(dims))
    return call(
        functools.partial(qkv_body, len(parts)),
        [shape((n, 3 * HD))] * 4,
        [gain, *parts, w],
        [pltpu.VMEM((n, D), BF), pltpu.VMEM((n, 4 * HD), BF)],
        grid=(3,),
        in_specs=[whole((1, D)), *(whole(part.shape) for part in parts),
                  pl.BlockSpec((1, D, 4 * HD), lambda c: (c, 0, 0))],
        out_specs=[whole((n, 3 * HD))] * 4,
        flops=2 * n * D * 12 * HD,
        size=7 << 20,
        limit=24 << 20,
    )


def attention_body(spread, first, lengths, *refs):
    qs, mine, theirs = refs[:4], refs[4], refs[5]
    given, outs = ((), refs[6:8]) if first else (refs[6:8], refs[8:12])
    q_all, k_all, v_all, held, tops_all, sem = refs[-6:]
    c, y, x, z = seats()
    quarter = 2 * lax.rem(y, 2) + c
    roll = lax.div(y, 2)
    length = lengths[roll]
    home = c == roll
    xs = [lax.rem(x + 4 + s, 4) for s in SHIFTS]
    twin = (lambda v: v) if first else (lambda v: v + 1 - 2 * lax.rem(v, 2))
    one, two = twin(jnp.where(home, y, 3 - y)), twin(jnp.where(home, 3 - y, y))

    def copies(act):
        for k in range(4):
            source = lax.rem(quarter + 4 - k, 4)
            for i in range(4):
                act(pltpu.make_async_copy(qs[k].at[i], q_all.at[source * 4 + xs[i]], sem))
        for slot, array in enumerate((mine, theirs)):
            for i in range(4):
                for p, shift in enumerate(spread):
                    at = (slot * 16 + xs[i] * 4 + lax.rem(z + 4 + shift, 4)) * QT
                    at = pl.ds(pl.multiple_of(at, QT), QT)
                    rows = pl.ds(p * QT, QT)
                    act(pltpu.make_async_copy(array.at[i, rows, pl.ds(0, HD)], k_all.at[at, :], sem))
                    act(pltpu.make_async_copy(array.at[i, rows, pl.ds(HD, HD)], v_all.at[at, pl.ds(0, HD)], sem))

    copies(lambda copy: copy.start())
    v_all[:, HD:] = jnp.ones((4096, HD), BF)
    if first:
        acc, peak = outs
        acc[...] = jnp.zeros((2048, 2 * HD), F32)
        peak[...] = jnp.full((2048, HD), -1e30, F32)
    else:
        acc, peak = refs[-8:-6]
        acc[...] = given[0][...]
        peak[...] = given[1][...]
    copies(lambda copy: copy.wait())

    high = lax.shift_right_logical(quarter, 1)
    blocks_in = lax.div(length + 7, 8)
    parts = [slice(rb * QT, (rb + 1) * QT) for rb in range(4)]
    count_one = jnp.where(one < blocks_in, 4 - one, 0)
    count = count_one + jnp.where(two < blocks_in, 4 - two, 0)

    def pair_at(p):
        slot = jnp.where(p >= count_one, 1, 0)
        block = jnp.where(p >= count_one, two, one)
        return slot, block, block + p - slot * count_one

    def bias(block, Y, kb, rb, half):
        seen = 2 * (block * 4 + kb) + half
        return jnp.where((seen <= 2 * (4 * Y + rb) + high) & (seen < length), 0.0, -1e30).astype(F32)

    def keys_at(slot, kb):
        return pl.ds(pl.multiple_of((slot * 4 + kb) * 512, 512), 512)

    def score(pair, kb, tops):
        slot, block, Y = pair
        q = q_all[pl.ds(Y * 4, 4)].reshape(512, HD)
        s = lax.dot_general(q, k_all[keys_at(slot, kb), :], (((1,), (1,)), ((), ())), preferred_element_type=F32)
        held[kb] = s
        made = []
        for rb in range(4):
            top = tops[rb]
            for half in range(2):
                piece = s[parts[rb], half * TOK_FRAME : (half + 1) * TOK_FRAME]
                top = jnp.maximum(top, jnp.maximum(piece[:, :HD], piece[:, HD:]) + bias(block, Y, kb, rb, half))
            made.append(top)
        return made

    def keep(tops):
        for rb in range(4):
            tops_all[parts[rb], :] = jnp.broadcast_to(jnp.max(tops[rb], axis=1, keepdims=True), (QT, HD))

    lowest = [jnp.full((QT, HD), -1e30, F32)] * 4
    tops = lowest
    for kb in range(4):
        tops = score(pair_at(0), kb, tops)
    keep(tops)

    def step(p, carry):
        slot, block, Y = pair_at(p)
        following = pair_at(jnp.minimum(p + 1, count - 1))
        rows_in = pl.ds(pl.multiple_of(Y * 512, 512), 512)
        before = peak[rows_in, :]
        now = jnp.maximum(before, tops_all[...])
        total = acc[rows_in, :] * jnp.exp2(before - now)[:, :1]
        peak[rows_in, :] = now
        tops = lowest
        for kb in range(4):
            rows = []
            for rb in range(4):
                row = [
                    jnp.exp2(held[kb, parts[rb], half * TOK_FRAME : (half + 1) * TOK_FRAME]
                             - (now[parts[rb], :1] - bias(block, Y, kb, rb, half))).astype(BF)
                    for half in range(2)
                ]
                rows.append(jnp.concatenate(row, axis=1))
            weights = jnp.concatenate(rows, axis=0)
            total = total + jnp.dot(weights, v_all[keys_at(slot, kb), :], preferred_element_type=F32)
            tops = score(following, kb, tops)
        acc[rows_in, :] = total
        keep(tops)
        return carry

    lax.fori_loop(0, count, step, 0)
    if first:
        return
    for k in range(4):
        source = lax.rem(quarter + 4 - k, 4)
        for i in range(4):
            at = pl.multiple_of((source * 4 + xs[i]) * QT, QT)
            rows_in = pl.ds(at, QT)
            outs[i][k] = (acc[rows_in, :HD] / acc[rows_in, HD:]).astype(BF)


def attention(lengths, qs, mine, theirs, spread, given=()):
    first = not given
    anyspace = pl.BlockSpec(memory_space=pl.ANY)
    whole = pl.BlockSpec(memory_space=VMEM)
    state = [shape((2048, 2 * HD), F32), shape((2048, HD), F32)]
    working = [] if first else [pltpu.VMEM((2048, 2 * HD), F32), pltpu.VMEM((2048, HD), F32)]
    outs = state if first else [shape((4, QT, HD))] * 4
    return call(
        functools.partial(attention_body, spread, first),
        outs,
        [lengths, *qs, mine, theirs, *given],
        [
            *working,
            pltpu.VMEM((16, QT, HD), BF),
            pltpu.VMEM((4096, HD), BF),
            pltpu.VMEM((4096, 2 * HD), BF),
            pltpu.VMEM((4, 512, 512), F32),
            pltpu.VMEM((512, HD), F32),
            pltpu.SemaphoreType.DMA,
        ],
        in_specs=[pl.BlockSpec(memory_space=SMEM)] + [anyspace] * 6 + [whole] * len(given),
        out_specs=[whole] * len(outs),
        flops=3 << 30,
        size=8 << 20,
        limit=24 << 20,
    )


def project_body(gain, rows, *refs):
    mixed_in, ws = refs[:4], refs[4:9]
    after, top, low, total, mixed, acc = refs[9:]
    step = pl.program_id(0)
    c, y, x, z = seats()

    @pl.when(step == 0)
    def _():
        for kk in range(4):
            z_from = lax.rem(y + 4 - kk, 4)
            for i, s in enumerate(SHIFTS):
                head = z_from * 4 + lax.rem(x + 4 - s, 4)
                mixed[:, pl.ds(pl.multiple_of(head * HD, HD), HD)] = mixed_in[kk][i]

    def term(slab, offset, w):
        at = pl.multiple_of(lax.rem(slab, 4) * 512 + offset, 256)
        return jnp.dot(mixed[:, pl.ds(at, w.shape[0])], w[...], preferred_element_type=F32)

    sums = term(z, 0, ws[0])
    sums = sums + term(z + 3 + 2 * c, 0, ws[1]) + term(z + 5 - 2 * c, 0, ws[2])
    sums = sums + term(z + 2, c * 256, ws[3]) + term(z + 2, (1 - c) * 256, ws[4])
    acc[:, pl.ds(pl.multiple_of(step * 512, 512), 512)] = sums

    @pl.when(step == 3)
    def _():
        rounded = (rows[...].astype(F32) + acc[...]).astype(BF)
        after[...] = rounded
        floats = rounded.astype(F32)
        normed2 = normalized(floats, gain[...])
        top[...] = normed2[: QT // 2]
        low[...] = normed2[QT // 2 :]
        total[...] = jnp.broadcast_to(jnp.sum(floats, axis=0, keepdims=True), (8, D))


def project(gain, rows, mixed_in, ws):
    whole = lambda dims: pl.BlockSpec(tuple(dims), lambda n: (0,) * len(dims))
    cut = lambda w: pl.BlockSpec((w.shape[0], 512), lambda n: (0, n))
    return call(
        project_body,
        [shape((QT, D)), shape((QT // 2, D)), shape((QT // 2, D)), shape((8, D), F32)],
        [gain, rows, *mixed_in, *ws],
        [pltpu.VMEM((QT, D), BF), pltpu.VMEM((QT, D), F32)],
        grid=(4,),
        in_specs=[whole((1, D)), whole((QT, D)), *(whole(m.shape) for m in mixed_in), *(cut(w) for w in ws)],
        out_specs=[whole((QT, D)), whole((QT // 2, D)), whole((QT // 2, D)), whole((8, D))],
        flops=2 * QT * D * D,
        size=9 << 20,
        limit=20 << 20,
    )


def pack_body(*refs):
    out = refs[4]
    for i in range(4):
        out[i] = refs[i][...]


def pack(pieces):
    n = pieces[0].shape[0]
    return call(
        pack_body, shape((4, n, 2 * HD)), pieces, grid=(1,),
        in_specs=[pl.BlockSpec((n, 2 * HD), lambda i: (0, 0))] * 4,
        out_specs=pl.BlockSpec((4, n, 2 * HD), lambda i: (0, 0, 0)),
        flops=1 << 22, size=n << 12, limit=8 << 20,
    )


def share_body(*refs):
    out = refs[6]
    home = seats()[0] == lax.div(seats()[1], 2)
    for pick, when in ((0, home), (1, jnp.logical_not(home))):

        @pl.when(when)
        def _():
            at = 0
            for g in range(3):
                part = refs[2 * g + pick]
                out[:, at : at + part.shape[1], :] = part[...]
                at += part.shape[1]


def final_body(after, own, one, two, out):
    out[...] = (after[...].astype(F32) + own[...] + one[...].astype(F32) + two[...].astype(F32)).astype(BF)


def queries_body(order, *refs):
    pieces, outs = refs[:12], refs[12:]
    _, y, _, z = seats()
    for k in range(4):
        turn = lax.rem(y + k + 4 - z, 4)
        for shift in range(4):
            group, part = order[shift]

            @pl.when(turn == shift)
            def _():
                for i in range(4):
                    outs[k][i] = pieces[group * 4 + i][part * QT : (part + 1) * QT, :]


def queries(groups, order):
    pieces = [piece for group in groups for piece in group]
    return call(
        functools.partial(queries_body, order), [shape((4, QT, HD))] * 4, pieces, grid=(1,),
        in_specs=[pl.BlockSpec((p.shape[0], HD), lambda i: (0, 2)) for p in pieces],
        out_specs=[pl.BlockSpec((4, QT, HD), lambda i: (0, 0, 0))] * 4,
        flops=1 << 22, size=1 << 20, limit=8 << 20,
    )


def heads_body(*refs):
    c, y, _, z = seats()
    quarter = 2 * lax.rem(y, 2) + c
    for kk in range(4):
        k = lax.rem(quarter + 8 - z - kk, 4)
        for i in range(4):
            refs[4 + kk][i] = refs[i][k]


def combine_body(part, to_right, to_left, left, right):
    half = QT // 2
    left[:half, :] = part[:half, :].astype(BF)
    left[half:, :] = (part[half:QT, :] + to_left[...].astype(F32)).astype(BF)
    right[:half, :] = (part[QT : QT + half, :] + to_right[...].astype(F32)).astype(BF)
    right[half:, :] = part[QT + half :, :].astype(BF)


def mlp_body(parts, cuts, *refs):
    rows, w_up, w_down = refs[:parts], refs[parts], refs[parts + 1]
    outs = refs[-4 - len(cuts) : -4]
    sums, inside, upper, acc = refs[-4:]
    step, n = pl.program_id(0), inside.shape[0]

    @pl.when(step == 0)
    def _():
        at = 0
        for part in rows:
            inside[at : at + part.shape[0], :] = part[...]
            at += part.shape[0]
        acc[...] = jnp.zeros_like(acc)

    hidden = jnp.dot(inside[...], w_up[...], preferred_element_type=F32)
    up = jax.nn.gelu(hidden, approximate=True).astype(BF)
    upper[:n, :] = up
    index = lax.broadcasted_iota(jnp.int32, (16, up.shape[1]), 0)
    extra = jnp.zeros((16, up.shape[1]), F32)
    for q in range(n // QT):
        whole = jnp.sum(up[q * QT : (q + 1) * QT, :].astype(F32), axis=0, keepdims=True)
        high = whole.astype(BF).astype(F32)
        extra = jnp.where(index == 2 * q, high, jnp.where(index == 2 * q + 1, whole - high, extra))
    upper[n:, :] = extra.astype(BF)
    acc[...] += jnp.dot(upper[...], w_down[...], preferred_element_type=F32)

    @pl.when(step == pl.num_programs(0) - 1)
    def _():
        at = 0
        for out in outs:
            out[...] = acc[at : at + out.shape[0], :].astype(out.dtype)
            at += out.shape[0]
        sums[...] = acc[n:, :]


def mlp(parts, w_up, w_down, cuts, after=()):
    n = sum(part.shape[0] for part in parts)
    ff = w_up.shape[1]
    block = 512
    whole = lambda dims: pl.BlockSpec(tuple(dims), lambda f: (0,) * len(dims))
    return call(
        functools.partial(mlp_body, len(parts), cuts),
        [*(shape((size, D), kind) for size, kind in cuts), shape((16, D), F32)],
        [*parts, w_up, w_down, *after],
        [pltpu.VMEM((n, D), BF), pltpu.VMEM((n + 16, block), BF), pltpu.VMEM((n + 16, D), F32)],
        grid=(ff // block,),
        in_specs=[*(whole(part.shape) for part in parts),
                  pl.BlockSpec((D, block), lambda f: (0, f)), pl.BlockSpec((block, D), lambda f: (f, 0)),
                  *([pl.BlockSpec(memory_space=pl.ANY)] * len(after))],
        out_specs=[*(whole((size, D)) for size, _ in cuts), whole((16, D))],
        flops=4 * n * D * ff,
        size=17 << 20,
        limit=28 << 20,
    )


def half_body(w, out, sem):
    rows = pl.ds(pl.multiple_of(lax.axis_index("dp").astype(jnp.int32) * 256, 256), 256)
    copy = pltpu.make_async_copy(w.at[rows, :], out, sem)
    copy.start()
    copy.wait()


def totals_body(near, far, mine, after, out):
    z = seats()[3]
    own = mine[0:1, :] + mine[1:2, :] + after[0:1, :]
    parts = ((0, own), (3, near[0:1, :] + near[1:2, :]), (1, near[2:3, :] + near[3:4, :]), (2, far[0:1, :] + far[1:2, :]))
    for frame in range(2):
        total = jnp.zeros((1, D), F32)
        for shift, part in parts:
            total = total + part * jnp.where(lax.rem(z + shift, 4) // 2 == frame, 1.0, 0.0)
        out[frame : frame + 1, :] = total


def stack_body(*refs):
    for i in range(4):
        refs[4][i] = refs[i][...]


def sum_body(*refs):
    refs[4][...] = refs[0][...] + refs[1][...] + refs[2][...] + refs[3][...]


def states_body(lengths, near, above, below, far, gain, bias, weight, out, means, states):
    c, y, x, _ = seats()
    length = lengths[c]
    for array, ys in ((near, 0), (below, -1), (above, 1), (far, 2)):
        for i, s in enumerate(SHIFTS):
            at = lax.rem(y + 4 + ys, 4) * 4 + lax.rem(x + 4 + s, 4)
            means[at] = array[i] * (1.0 / TOK_FRAME)
    state = jnp.zeros((1, D), F32)
    for frame in range(FRAMES):
        mean = means[frame // 2, frame % 2 : frame % 2 + 1, :]
        gate = jax.nn.sigmoid(mean * gain[...] + bias[...])
        state = jnp.where(frame < length, gate * state + (1.0 - gate) * mean, state)
        states[frame : frame + 1, :] = state
    values = jnp.sum(states[...] * weight[...], axis=1, keepdims=True)
    index = lax.broadcasted_iota(jnp.int32, (FRAMES, HD), 0)
    out[...] = jnp.where(index < length, values, 0.0)


def advantages_body(lengths, mine, theirs, first, second):
    c, y, x, _ = seats()
    length, length_other = lengths[c], lengths[1 - c]
    index = lax.broadcasted_iota(jnp.int32, (FRAMES, HD), 0)

    def gap_of(values, size):
        final = jnp.sum(jnp.where(index == size - 1, values, 0.0), axis=0, keepdims=True)
        return jnp.where(index < size, final - values, 0.0)

    gap, gap_other = gap_of(mine[...], length), gap_of(theirs[...], length_other)
    count = (length + length_other).astype(F32)
    summed = lambda v: jnp.sum(v, axis=0, keepdims=True)
    mean = (summed(gap) + summed(gap_other)) / count
    centered = jnp.where(index < length, gap - mean, 0.0)
    centered_other = jnp.where(index < length_other, gap_other - mean, 0.0)
    variance = (summed(centered * centered) + summed(centered_other * centered_other)) / count
    scaled = jnp.where(index < length, centered * lax.rsqrt(variance + 1e-05), 0.0)
    at = (y * 4 + x) * 2
    lane = lax.broadcasted_iota(jnp.int32, (1, HD), 1)

    def picked(values):
        one, two = (summed(jnp.where(index == at + e, values, 0.0)) for e in (0, 1))
        return jnp.where(lane == 0, one, two)[:, :2]

    first[...] = picked(mine[...])
    second[...] = picked(scaled)


def local(tokens, attn_gain, w_qkv, w_out, mlp_gain, w_up, w_down, pool_gain, pool_bias, value_weight, valid_frames):
    rows = tokens[0]
    line = lambda v: v.reshape(1, D)

    from_left = moved(rows, "tensor", 1)
    from_right = moved(rows, "tensor", -1)
    far_top = moved(from_left[:64], "tensor", 1)
    far_low = moved(from_right[64:], "tensor", -1)
    groups = (((rows,), (0,)), ((from_left, from_right), (-1, 1)), ((far_top, far_low), (2,)))
    spread = tuple(shift for group in groups for shift in group[1])

    pa_pairs, pb_pairs = [], []
    for core in range(2):
        for yy in range(4):
            if yy // 2 == core:
                pa_pairs.append((flat(core, yy), flat(core, yy ^ 1)))
            else:
                pa_pairs.append((flat(core, yy), flat(1 - core, 3 - yy)))
                pb_pairs.append((flat(core, yy), flat(core, yy ^ 1)))
    swap = [(0, 1), (1, 0)]

    chunks, held, order = [], [], {}
    for g, (parts, shifts) in enumerate(groups):
        made = qkv_of(line(attn_gain), parts, w_qkv)
        got = [made[0], moved(made[1], "x", 1), moved(made[3], "x", -1), moved(made[2], "x", 2)]
        held.append(got)
        block = pack(got)
        pa = lax.ppermute(block, ("dp", "y"), pa_pairs)
        pb = lax.ppermute(pa, ("dp", "y"), pb_pairs)
        chunks.append((block, pa, pb))
        for p, shift in enumerate(shifts):
            order[shift % 4] = (g, p)
    qs = []
    for k, part in enumerate(queries(held, order)):
        pairs = []
        for core in range(2):
            for yy in range(4):
                j = (yy + k) % 4
                pairs.append((flat(core, yy), flat(j % 2, 2 * core + j // 2)))
        qs.append(lax.ppermute(part, ("dp", "y"), pairs))

    shared = []
    for b in range(2):
        mine = call(
            share_body, shape((4, 512, 2 * HD)), [chunk[b + i] for chunk in chunks for i in range(2)],
            flops=1 << 24, size=2 << 20, limit=10 << 20,
        )
        shared.append((mine, lax.ppermute(mine, "dp", swap)))
    state = attention(valid_frames, qs, *shared[0], spread)
    outs = attention(valid_frames, qs, *shared[1], spread, tuple(state))

    w_first, _, _ = lax.optimization_barrier((w_out, far_low, far_top))
    pairs = [(4 * core + zz, 4 * core + (zz + 1 - 2 * core) % 4) for core in range(2) for zz in range(4)]
    w_near = lax.ppermute(w_first, ("dp", "tensor"), pairs)
    w_half = call(
        half_body, shape((256, D)), [w_near], [pltpu.SemaphoreType.DMA],
        in_specs=[pl.BlockSpec(memory_space=pl.ANY)], flops=1 << 22, size=2 << 20, limit=4 << 20,
    )
    w_far = lax.ppermute(w_half, ("dp", "tensor"), pairs)
    ws = [w_out, w_near, lax.ppermute(w_near, "dp", swap), w_far, lax.ppermute(w_far, "dp", swap)]

    heads = [outs[0], moved(outs[1], "x", -1), moved(outs[2], "x", 1), moved(outs[3], "x", 2)]
    heads = call(heads_body, [shape((4, QT, HD))] * 4, heads, flops=1 << 22, size=1 << 20, limit=8 << 20)
    mixed_in = []
    for kk, part in enumerate(heads):
        pairs = []
        for core in range(2):
            for yy in range(4):
                for zz in range(4):
                    j = 2 * (yy % 2) + core
                    pairs.append((flat(core, yy, zz), flat(yy // 2, (zz + kk) % 4, j)))
        mixed_in.append(lax.ppermute(part, ("dp", "y", "tensor"), pairs))
    after, top, low, after_sum = project(line(mlp_gain), rows, mixed_in, ws)

    left_top = moved(top, "tensor", 1)
    right_low = moved(low, "tensor", -1)
    opposite_top = moved(left_top, "tensor", 1)
    opposite_low = moved(right_low, "tensor", -1)
    left_low = moved(low, "tensor", 1)
    right_top = moved(top, "tensor", -1)
    own_part, own_sums = mlp((top, low), w_up, w_down, ((128, F32),))
    far_upper, far_lower, far_sums = mlp((opposite_top, opposite_low), w_up, w_down, ((64, BF), (64, BF)))
    near_in = (left_top, left_low, right_top, right_low)
    side_part, near_sums = mlp(near_in, w_up, w_down, ((256, F32),))
    to_right = moved(far_upper, "tensor", 1)
    to_left = moved(far_lower, "tensor", -1)
    for_left, for_right = call(
        combine_body, [shape((QT, D))] * 2, [side_part, to_right, to_left], grid=(1,),
        in_specs=[pl.BlockSpec((2 * QT, D), lambda i: (0, 0)), *([pl.BlockSpec((QT // 2, D), lambda i: (0, 0))] * 2)],
        out_specs=[pl.BlockSpec((QT, D), lambda i: (0, 0))] * 2, flops=1 << 22, size=4 << 20, limit=16 << 20,
    )
    sum_one = moved(for_right, "tensor", 1)
    sum_two = moved(for_left, "tensor", -1)
    block = lambda n: pl.BlockSpec((n, D), lambda i: (i, 0))
    hidden = call(
        final_body, shape((QT, D)), [after, own_part, sum_one, sum_two], grid=(2,),
        in_specs=[block(64)] * 4, out_specs=block(64), flops=1 << 20, size=3 << 20, limit=8 << 20,
    )

    totals = call(
        totals_body, shape((2, D), F32), [near_sums, far_sums, own_sums, after_sum], flops=1 << 16, size=1 << 19, limit=4 << 20,
    )
    rest = [moved(totals, "tensor", s) for s in (1, -1, 2)]
    totals = call(sum_body, shape((2, D), F32), [totals, *rest], flops=1 << 14, size=1 << 17, limit=4 << 20)
    rest = [moved(totals, "x", s) for s in (1, -1, 2)]
    over_x = call(stack_body, shape((4, 2, D), F32), [totals, *rest], flops=1 << 14, size=1 << 17, limit=4 << 20)
    below, above, across = (moved(over_x, "y", s) for s in (1, -1, 2))
    values = call(
        states_body,
        shape((FRAMES, HD), F32),
        [valid_frames, over_x, above, below, across, line(pool_gain), line(pool_bias), line(value_weight)],
        [pltpu.VMEM((16, 2, D), F32), pltpu.VMEM((FRAMES, D), F32)],
        in_specs=[pl.BlockSpec(memory_space=SMEM)] + [pl.BlockSpec(memory_space=VMEM)] * 7,
        flops=1 << 20,
        size=1 << 20,
        limit=8 << 20,
    )
    other_values = lax.ppermute(values, "dp", swap)
    frame_values, advantages = call(
        advantages_body,
        [shape((1, 2), F32)] * 2,
        [valid_frames, values, other_values],
        in_specs=[pl.BlockSpec(memory_space=SMEM)] + [pl.BlockSpec(memory_space=VMEM)] * 2,
        flops=1 << 14,
        size=1 << 15,
        limit=4 << 20,
    )
    return hidden[None], frame_values, advantages


def solution(mesh):
    fine = Mesh(mesh.devices.reshape(2, 4, 4, 4), ("dp", "y", "x", "tensor"))
    token_spec = P("dp", ("y", "x", "tensor"), None)
    in_specs = (
        token_spec,
        P(),
        P(None, None, "tensor"),
        P("tensor", None),
        P(),
        P(None, "tensor"),
        P("tensor", None),
        P(),
        P(),
        P(),
        P(),
    )
    out_specs = (token_spec, P("dp", ("y", "x")), P("dp", ("y", "x")))
    return jax.shard_map(local, mesh=fine, in_specs=in_specs, out_specs=out_specs, check_vma=False)
```

```python
import functools
import math

import jax
import jax.numpy as jnp
from jax import lax
from jax.experimental import pallas as pl
from jax.experimental.pallas import tpu as pltpu
from jax.sharding import Mesh, PartitionSpec as P


D = 2048
HD = 128
QT = 128
FRAMES = 32
TOK_FRAME = 256
BF = jnp.bfloat16
F32 = jnp.float32
QSCALE = math.log2(math.e) / math.sqrt(HD)
SHIFTS = (0, -1, 1, 2)
VMEM = pltpu.VMEM
SMEM = pltpu.SMEM


def ring(shift):
    return [(i, (i + shift) % 4) for i in range(4)]


def moved(array, axis, shift):
    return lax.ppermute(array, axis, ring(shift))


def flat(*digits):
    sizes = {2: (2, 4), 3: (2, 4, 4)}[len(digits)]
    at = 0
    for digit, size in zip(digits, sizes):
        at = at * size + digit
    return at


def seats():
    return tuple(lax.axis_index(name).astype(jnp.int32) for name in ("dp", "y", "x", "tensor"))


def call(body, out, ins, scratch=(), grid=None, in_specs=None, out_specs=None, flops=0, size=0, limit=None):
    single = not isinstance(out, (list, tuple))
    outs = [out] if single else list(out)
    whole = pl.BlockSpec(memory_space=VMEM)
    kwargs = {} if grid is None else {"grid": grid}
    return pl.pallas_call(
        body,
        out_shape=out if single else outs,
        in_specs=in_specs or [whole] * len(ins),
        out_specs=out_specs or (whole if single else [whole] * len(outs)),
        scratch_shapes=list(scratch),
        compiler_params=pltpu.CompilerParams(vmem_limit_bytes=limit),
        cost_estimate=pl.CostEstimate(flops=flops, bytes_accessed=size, transcendentals=0),
        **kwargs,
    )(*ins)


def shape(dims, kind=BF):
    return jax.ShapeDtypeStruct(tuple(dims), kind)


def normalized(floats, gain):
    square = jnp.mean(floats * floats, axis=-1, keepdims=True)
    return (floats * lax.rsqrt(square + 1e-05) * gain).astype(BF)


def qkv_body(parts, gain, *refs):
    place = seats()
    rows, w, outs, normed, made = refs[:parts], refs[parts], refs[parts + 1 : parts + 5], refs[-2], refs[-1]
    step = pl.program_id(0)

    @pl.when(step == 0)
    def _():
        at = 0
        for part in rows:
            n = part.shape[0]
            normed[at : at + n, :] = normalized(part[...].astype(F32), gain[...])
            at += n

    product = jnp.dot(normed[...], w[0], preferred_element_type=F32)
    product = product * jnp.where(step == 0, QSCALE, 1.0)
    made[...] = product.astype(BF)
    slot = lax.rem(step + 2, 3)
    for rel in range(4):
        head = lax.rem(place[2] + rel, 4)
        outs[rel][:, pl.ds(pl.multiple_of(slot * HD, HD), HD)] = made[:, pl.ds(pl.multiple_of(head * HD, HD), HD)]


def qkv_of(gain, parts, w):
    n = sum(part.shape[0] for part in parts)
    whole = lambda dims: pl.BlockSpec(tuple(dims), lambda c: (0,) * len(dims))
    return call(
        functools.partial(qkv_body, len(parts)),
        [shape((n, 3 * HD))] * 4,
        [gain, *parts, w],
        [pltpu.VMEM((n, D), BF), pltpu.VMEM((n, 4 * HD), BF)],
        grid=(3,),
        in_specs=[whole((1, D)), *(whole(part.shape) for part in parts),
                  pl.BlockSpec((1, D, 4 * HD), lambda c: (c, 0, 0))],
        out_specs=[whole((n, 3 * HD))] * 4,
        flops=2 * n * D * 12 * HD,
        size=7 << 20,
        limit=24 << 20,
    )


def attention_body(spread, first, lengths, *refs):
    qs, mine, theirs = refs[:4], refs[4], refs[5]
    given, outs = ((), refs[6:8]) if first else (refs[6:8], refs[8:12])
    q_all, k_all, v_all, held, tops_all, sem = refs[-6:]
    c, y, x, z = seats()
    quarter = 2 * lax.rem(y, 2) + c
    roll = lax.div(y, 2)
    length = lengths[roll]
    home = c == roll
    xs = [lax.rem(x + 4 + s, 4) for s in SHIFTS]
    twin = (lambda v: v) if first else (lambda v: v + 1 - 2 * lax.rem(v, 2))
    one, two = twin(jnp.where(home, y, 3 - y)), twin(jnp.where(home, 3 - y, y))

    def copies(act):
        for k in range(4):
            source = lax.rem(quarter + 4 - k, 4)
            for i in range(4):
                act(pltpu.make_async_copy(qs[k].at[i], q_all.at[source * 4 + xs[i]], sem))
        for slot, array in enumerate((mine, theirs)):
            for i in range(4):
                for p, shift in enumerate(spread):
                    at = (slot * 16 + xs[i] * 4 + lax.rem(z + 4 + shift, 4)) * QT
                    at = pl.ds(pl.multiple_of(at, QT), QT)
                    rows = pl.ds(p * QT, QT)
                    act(pltpu.make_async_copy(array.at[i, rows, pl.ds(0, HD)], k_all.at[at, :], sem))
                    act(pltpu.make_async_copy(array.at[i, rows, pl.ds(HD, HD)], v_all.at[at, pl.ds(0, HD)], sem))

    copies(lambda copy: copy.start())
    v_all[:, HD:] = jnp.ones((4096, HD), BF)
    if first:
        acc, peak = outs
        acc[...] = jnp.zeros((2048, 2 * HD), F32)
        peak[...] = jnp.full((2048, HD), -1e30, F32)
    else:
        acc, peak = refs[-8:-6]
        acc[...] = given[0][...]
        peak[...] = given[1][...]
    copies(lambda copy: copy.wait())

    high = lax.shift_right_logical(quarter, 1)
    blocks_in = lax.div(length + 7, 8)
    parts = [slice(rb * QT, (rb + 1) * QT) for rb in range(4)]
    count_one = jnp.where(one < blocks_in, 4 - one, 0)
    count = count_one + jnp.where(two < blocks_in, 4 - two, 0)

    def pair_at(p):
        slot = jnp.where(p >= count_one, 1, 0)
        block = jnp.where(p >= count_one, two, one)
        return slot, block, block + p - slot * count_one

    def bias(block, Y, kb, rb, half):
        seen = 2 * (block * 4 + kb) + half
        return jnp.where((seen <= 2 * (4 * Y + rb) + high) & (seen < length), 0.0, -1e30).astype(F32)

    def keys_at(slot, kb):
        return pl.ds(pl.multiple_of((slot * 4 + kb) * 512, 512), 512)

    def score(pair, kb, tops):
        slot, block, Y = pair
        q = q_all[pl.ds(Y * 4, 4)].reshape(512, HD)
        s = lax.dot_general(q, k_all[keys_at(slot, kb), :], (((1,), (1,)), ((), ())), preferred_element_type=F32)
        held[kb] = s
        made = []
        for rb in range(4):
            top = tops[rb]
            for half in range(2):
                piece = s[parts[rb], half * TOK_FRAME : (half + 1) * TOK_FRAME]
                top = jnp.maximum(top, jnp.maximum(piece[:, :HD], piece[:, HD:]) + bias(block, Y, kb, rb, half))
            made.append(top)
        return made

    def keep(tops):
        for rb in range(4):
            tops_all[parts[rb], :] = jnp.broadcast_to(jnp.max(tops[rb], axis=1, keepdims=True), (QT, HD))

    lowest = [jnp.full((QT, HD), -1e30, F32)] * 4
    tops = lowest
    for kb in range(4):
        tops = score(pair_at(0), kb, tops)
    keep(tops)

    def step(p, carry):
        slot, block, Y = pair_at(p)
        following = pair_at(jnp.minimum(p + 1, count - 1))
        rows_in = pl.ds(pl.multiple_of(Y * 512, 512), 512)
        before = peak[rows_in, :]
        now = jnp.maximum(before, tops_all[...])
        total = acc[rows_in, :] * jnp.exp2(before - now)[:, :1]
        peak[rows_in, :] = now
        tops = lowest
        for kb in range(4):
            rows = []
            for rb in range(4):
                row = [
                    jnp.exp2(held[kb, parts[rb], half * TOK_FRAME : (half + 1) * TOK_FRAME]
                             - (now[parts[rb], :1] - bias(block, Y, kb, rb, half))).astype(BF)
                    for half in range(2)
                ]
                rows.append(jnp.concatenate(row, axis=1))
            weights = jnp.concatenate(rows, axis=0)
            total = total + jnp.dot(weights, v_all[keys_at(slot, kb), :], preferred_element_type=F32)
            tops = score(following, kb, tops)
        acc[rows_in, :] = total
        keep(tops)
        return carry

    lax.fori_loop(0, count, step, 0)
    if first:
        return
    for k in range(4):
        source = lax.rem(quarter + 4 - k, 4)
        for i in range(4):
            at = pl.multiple_of((source * 4 + xs[i]) * QT, QT)
            rows_in = pl.ds(at, QT)
            outs[i][k] = (acc[rows_in, :HD] / acc[rows_in, HD:]).astype(BF)


def attention(lengths, qs, mine, theirs, spread, given=()):
    first = not given
    anyspace = pl.BlockSpec(memory_space=pl.ANY)
    whole = pl.BlockSpec(memory_space=VMEM)
    state = [shape((2048, 2 * HD), F32), shape((2048, HD), F32)]
    working = [] if first else [pltpu.VMEM((2048, 2 * HD), F32), pltpu.VMEM((2048, HD), F32)]
    outs = state if first else [shape((4, QT, HD))] * 4
    return call(
        functools.partial(attention_body, spread, first),
        outs,
        [lengths, *qs, mine, theirs, *given],
        [
            *working,
            pltpu.VMEM((16, QT, HD), BF),
            pltpu.VMEM((4096, HD), BF),
            pltpu.VMEM((4096, 2 * HD), BF),
            pltpu.VMEM((4, 512, 512), F32),
            pltpu.VMEM((512, HD), F32),
            pltpu.SemaphoreType.DMA,
        ],
        in_specs=[pl.BlockSpec(memory_space=SMEM)] + [anyspace] * 6 + [whole] * len(given),
        out_specs=[whole] * len(outs),
        flops=3 << 30,
        size=8 << 20,
        limit=24 << 20,
    )


def project_body(gain, rows, *refs):
    mixed_in, ws = refs[:4], refs[4:9]
    after, top, low, total, mixed, acc = refs[9:]
    step = pl.program_id(0)
    c, y, x, z = seats()

    @pl.when(step == 0)
    def _():
        for kk in range(4):
            z_from = lax.rem(y + 4 - kk, 4)
            for i, s in enumerate(SHIFTS):
                head = z_from * 4 + lax.rem(x + 4 - s, 4)
                mixed[:, pl.ds(pl.multiple_of(head * HD, HD), HD)] = mixed_in[kk][i]

    def term(slab, offset, w):
        at = pl.multiple_of(lax.rem(slab, 4) * 512 + offset, 256)
        return jnp.dot(mixed[:, pl.ds(at, w.shape[0])], w[...], preferred_element_type=F32)

    sums = term(z, 0, ws[0])
    sums = sums + term(z + 3 + 2 * c, 0, ws[1]) + term(z + 5 - 2 * c, 0, ws[2])
    sums = sums + term(z + 2, c * 256, ws[3]) + term(z + 2, (1 - c) * 256, ws[4])
    acc[:, pl.ds(pl.multiple_of(step * 512, 512), 512)] = sums

    @pl.when(step == 3)
    def _():
        rounded = (rows[...].astype(F32) + acc[...]).astype(BF)
        after[...] = rounded
        floats = rounded.astype(F32)
        normed2 = normalized(floats, gain[...])
        top[...] = normed2[: QT // 2]
        low[...] = normed2[QT // 2 :]
        total[...] = jnp.broadcast_to(jnp.sum(floats, axis=0, keepdims=True), (8, D))


def project(gain, rows, mixed_in, ws):
    whole = lambda dims: pl.BlockSpec(tuple(dims), lambda n: (0,) * len(dims))
    cut = lambda w: pl.BlockSpec((w.shape[0], 512), lambda n: (0, n))
    return call(
        project_body,
        [shape((QT, D)), shape((QT // 2, D)), shape((QT // 2, D)), shape((8, D), F32)],
        [gain, rows, *mixed_in, *ws],
        [pltpu.VMEM((QT, D), BF), pltpu.VMEM((QT, D), F32)],
        grid=(4,),
        in_specs=[whole((1, D)), whole((QT, D)), *(whole(m.shape) for m in mixed_in), *(cut(w) for w in ws)],
        out_specs=[whole((QT, D)), whole((QT // 2, D)), whole((QT // 2, D)), whole((8, D))],
        flops=2 * QT * D * D,
        size=9 << 20,
        limit=20 << 20,
    )


def pack_body(*refs):
    out = refs[4]
    for i in range(4):
        out[i] = refs[i][...]


def pack(pieces):
    n = pieces[0].shape[0]
    return call(
        pack_body, shape((4, n, 2 * HD)), pieces, grid=(1,),
        in_specs=[pl.BlockSpec((n, 2 * HD), lambda i: (0, 0))] * 4,
        out_specs=pl.BlockSpec((4, n, 2 * HD), lambda i: (0, 0, 0)),
        flops=1 << 22, size=n << 12, limit=8 << 20,
    )


def share_body(*refs):
    out = refs[6]
    home = seats()[0] == lax.div(seats()[1], 2)
    for pick, when in ((0, home), (1, jnp.logical_not(home))):

        @pl.when(when)
        def _():
            at = 0
            for g in range(3):
                part = refs[2 * g + pick]
                out[:, at : at + part.shape[1], :] = part[...]
                at += part.shape[1]


def final_body(after, own, *refs):
    total = after[...].astype(F32) + own[...]
    for part in refs[:3]:
        total = total + part[...].astype(F32)
    refs[3][...] = total.astype(BF)


def queries_body(order, *refs):
    pieces, outs = refs[:12], refs[12:]
    _, y, _, z = seats()
    for k in range(4):
        turn = lax.rem(y + k + 4 - z, 4)
        for shift in range(4):
            group, part = order[shift]

            @pl.when(turn == shift)
            def _():
                for i in range(4):
                    outs[k][i] = pieces[group * 4 + i][part * QT : (part + 1) * QT, :]


def queries(groups, order):
    pieces = [piece for group in groups for piece in group]
    return call(
        functools.partial(queries_body, order), [shape((4, QT, HD))] * 4, pieces, grid=(1,),
        in_specs=[pl.BlockSpec((p.shape[0], HD), lambda i: (0, 2)) for p in pieces],
        out_specs=[pl.BlockSpec((4, QT, HD), lambda i: (0, 0, 0))] * 4,
        flops=1 << 22, size=1 << 20, limit=8 << 20,
    )


def heads_body(*refs):
    c, y, _, z = seats()
    quarter = 2 * lax.rem(y, 2) + c
    for kk in range(4):
        k = lax.rem(quarter + 8 - z - kk, 4)
        for i in range(4):
            refs[4 + kk][i] = refs[i][k]


def mlp_body(parts, cuts, *refs):
    rows, w_up, w_down = refs[:parts], refs[parts], refs[parts + 1]
    outs = refs[-4 - len(cuts) : -4]
    sums, inside, upper, acc = refs[-4:]
    step, n = pl.program_id(0), inside.shape[0]

    @pl.when(step == 0)
    def _():
        at = 0
        for part in rows:
            inside[at : at + part.shape[0], :] = part[...]
            at += part.shape[0]
        acc[...] = jnp.zeros_like(acc)

    hidden = jnp.dot(inside[...], w_up[...], preferred_element_type=F32)
    up = jax.nn.gelu(hidden, approximate=True).astype(BF)
    upper[:n, :] = up
    index = lax.broadcasted_iota(jnp.int32, (16, up.shape[1]), 0)
    extra = jnp.zeros((16, up.shape[1]), F32)
    for q in range(n // QT):
        whole = jnp.sum(up[q * QT : (q + 1) * QT, :].astype(F32), axis=0, keepdims=True)
        high = whole.astype(BF).astype(F32)
        extra = jnp.where(index == 2 * q, high, jnp.where(index == 2 * q + 1, whole - high, extra))
    upper[n:, :] = extra.astype(BF)
    acc[...] += jnp.dot(upper[...], w_down[...], preferred_element_type=F32)

    @pl.when(step == pl.num_programs(0) - 1)
    def _():
        at = 0
        for out in outs:
            out[...] = acc[at : at + out.shape[0], :].astype(out.dtype)
            at += out.shape[0]
        sums[...] = acc[n:, :]


def mlp(parts, w_up, w_down, cuts, after=()):
    n = sum(part.shape[0] for part in parts)
    ff = w_up.shape[1]
    block = 512
    whole = lambda dims: pl.BlockSpec(tuple(dims), lambda f: (0,) * len(dims))
    return call(
        functools.partial(mlp_body, len(parts), cuts),
        [*(shape((size, D), kind) for size, kind in cuts), shape((16, D), F32)],
        [*parts, w_up, w_down, *after],
        [pltpu.VMEM((n, D), BF), pltpu.VMEM((n + 16, block), BF), pltpu.VMEM((n + 16, D), F32)],
        grid=(ff // block,),
        in_specs=[*(whole(part.shape) for part in parts),
                  pl.BlockSpec((D, block), lambda f: (0, f)), pl.BlockSpec((block, D), lambda f: (f, 0)),
                  *([pl.BlockSpec(memory_space=pl.ANY)] * len(after))],
        out_specs=[*(whole((size, D)) for size, _ in cuts), whole((16, D))],
        flops=4 * n * D * ff,
        size=17 << 20,
        limit=28 << 20,
    )


def half_body(w, out, sem):
    rows = pl.ds(pl.multiple_of(lax.axis_index("dp").astype(jnp.int32) * 256, 256), 256)
    copy = pltpu.make_async_copy(w.at[rows, :], out, sem)
    copy.start()
    copy.wait()


def totals_body(near, far, mine, after, out):
    z = seats()[3]
    own = mine[0:1, :] + mine[1:2, :] + after[0:1, :]
    parts = ((0, own), (3, near[0:1, :] + near[1:2, :]), (1, near[2:3, :] + near[3:4, :]), (2, far[0:1, :] + far[1:2, :]))
    for frame in range(2):
        total = jnp.zeros((1, D), F32)
        for shift, part in parts:
            total = total + part * jnp.where(lax.rem(z + shift, 4) // 2 == frame, 1.0, 0.0)
        out[frame : frame + 1, :] = total


def stack_body(*refs):
    for i in range(4):
        refs[4][i] = refs[i][...]


def sum_body(*refs):
    refs[4][...] = refs[0][...] + refs[1][...] + refs[2][...] + refs[3][...]


def states_body(lengths, near, above, below, far, gain, bias, weight, out, means, states):
    c, y, x, _ = seats()
    length = lengths[c]
    for array, ys in ((near, 0), (below, -1), (above, 1), (far, 2)):
        for i, s in enumerate(SHIFTS):
            at = lax.rem(y + 4 + ys, 4) * 4 + lax.rem(x + 4 + s, 4)
            means[at] = array[i] * (1.0 / TOK_FRAME)
    state = jnp.zeros((1, D), F32)
    for frame in range(FRAMES):
        mean = means[frame // 2, frame % 2 : frame % 2 + 1, :]
        gate = jax.nn.sigmoid(mean * gain[...] + bias[...])
        state = jnp.where(frame < length, gate * state + (1.0 - gate) * mean, state)
        states[frame : frame + 1, :] = state
    values = jnp.sum(states[...] * weight[...], axis=1, keepdims=True)
    index = lax.broadcasted_iota(jnp.int32, (FRAMES, HD), 0)
    out[...] = jnp.where(index < length, values, 0.0)


def advantages_body(lengths, mine, theirs, first, second):
    c, y, x, _ = seats()
    length, length_other = lengths[c], lengths[1 - c]
    index = lax.broadcasted_iota(jnp.int32, (FRAMES, HD), 0)

    def gap_of(values, size):
        final = jnp.sum(jnp.where(index == size - 1, values, 0.0), axis=0, keepdims=True)
        return jnp.where(index < size, final - values, 0.0)

    gap, gap_other = gap_of(mine[...], length), gap_of(theirs[...], length_other)
    count = (length + length_other).astype(F32)
    summed = lambda v: jnp.sum(v, axis=0, keepdims=True)
    mean = (summed(gap) + summed(gap_other)) / count
    centered = jnp.where(index < length, gap - mean, 0.0)
    centered_other = jnp.where(index < length_other, gap_other - mean, 0.0)
    variance = (summed(centered * centered) + summed(centered_other * centered_other)) / count
    scaled = jnp.where(index < length, centered * lax.rsqrt(variance + 1e-05), 0.0)
    at = (y * 4 + x) * 2
    lane = lax.broadcasted_iota(jnp.int32, (1, HD), 1)

    def picked(values):
        one, two = (summed(jnp.where(index == at + e, values, 0.0)) for e in (0, 1))
        return jnp.where(lane == 0, one, two)[:, :2]

    first[...] = picked(mine[...])
    second[...] = picked(scaled)


def local(tokens, attn_gain, w_qkv, w_out, mlp_gain, w_up, w_down, pool_gain, pool_bias, value_weight, valid_frames):
    rows = tokens[0]
    line = lambda v: v.reshape(1, D)

    from_left = moved(rows, "tensor", 1)
    from_right = moved(rows, "tensor", -1)
    far_top = moved(from_left[:64], "tensor", 1)
    far_low = moved(from_right[64:], "tensor", -1)
    groups = (((rows,), (0,)), ((from_left, from_right), (-1, 1)), ((far_top, far_low), (2,)))
    spread = tuple(shift for group in groups for shift in group[1])

    pa_pairs, pb_pairs = [], []
    for core in range(2):
        for yy in range(4):
            if yy // 2 == core:
                pa_pairs.append((flat(core, yy), flat(core, yy ^ 1)))
            else:
                pa_pairs.append((flat(core, yy), flat(1 - core, 3 - yy)))
                pb_pairs.append((flat(core, yy), flat(core, yy ^ 1)))
    swap = [(0, 1), (1, 0)]

    chunks, held, order = [], [], {}
    for g, (parts, shifts) in enumerate(groups):
        made = qkv_of(line(attn_gain), parts, w_qkv)
        got = [made[0], moved(made[1], "x", 1), moved(made[3], "x", -1), moved(made[2], "x", 2)]
        held.append(got)
        block = pack(got)
        pa = lax.ppermute(block, ("dp", "y"), pa_pairs)
        pb = lax.ppermute(pa, ("dp", "y"), pb_pairs)
        chunks.append((block, pa, pb))
        for p, shift in enumerate(shifts):
            order[shift % 4] = (g, p)
    qs = []
    for k, part in enumerate(queries(held, order)):
        pairs = []
        for core in range(2):
            for yy in range(4):
                j = (yy + k) % 4
                pairs.append((flat(core, yy), flat(j % 2, 2 * core + j // 2)))
        qs.append(lax.ppermute(part, ("dp", "y"), pairs))

    shared = []
    for b in range(2):
        mine = call(
            share_body, shape((4, 512, 2 * HD)), [chunk[b + i] for chunk in chunks for i in range(2)],
            flops=1 << 24, size=2 << 20, limit=10 << 20,
        )
        shared.append((mine, lax.ppermute(mine, "dp", swap)))
    state = attention(valid_frames, qs, *shared[0], spread)
    outs = attention(valid_frames, qs, *shared[1], spread, tuple(state))

    w_first, _, _ = lax.optimization_barrier((w_out, far_low, far_top))
    pairs = [(4 * core + zz, 4 * core + (zz + 1 - 2 * core) % 4) for core in range(2) for zz in range(4)]
    w_near = lax.ppermute(w_first, ("dp", "tensor"), pairs)
    w_half = call(
        half_body, shape((256, D)), [w_near], [pltpu.SemaphoreType.DMA],
        in_specs=[pl.BlockSpec(memory_space=pl.ANY)], flops=1 << 22, size=2 << 20, limit=4 << 20,
    )
    w_far = lax.ppermute(w_half, ("dp", "tensor"), pairs)
    ws = [w_out, w_near, lax.ppermute(w_near, "dp", swap), w_far, lax.ppermute(w_far, "dp", swap)]

    heads = [outs[0], moved(outs[1], "x", -1), moved(outs[2], "x", 1), moved(outs[3], "x", 2)]
    heads = call(heads_body, [shape((4, QT, HD))] * 4, heads, flops=1 << 22, size=1 << 20, limit=8 << 20)
    mixed_in = []
    for kk, part in enumerate(heads):
        pairs = []
        for core in range(2):
            for yy in range(4):
                for zz in range(4):
                    j = 2 * (yy % 2) + core
                    pairs.append((flat(core, yy, zz), flat(yy // 2, (zz + kk) % 4, j)))
        mixed_in.append(lax.ppermute(part, ("dp", "y", "tensor"), pairs))
    after, top, low, after_sum = project(line(mlp_gain), rows, mixed_in, ws)

    left_top = moved(top, "tensor", 1)
    right_low = moved(low, "tensor", -1)
    opposite_top = moved(left_top, "tensor", 1)
    opposite_low = moved(right_low, "tensor", -1)
    left_low = moved(low, "tensor", 1)
    right_top = moved(top, "tensor", -1)
    own_part, own_sums = mlp((top, low), w_up, w_down, ((128, F32),))
    far_part, far_sums = mlp((opposite_top, opposite_low), w_up, w_down, ((128, BF),))
    near_in = (left_top, left_low, right_top, right_low)
    for_left, for_right, near_sums = mlp(near_in, w_up, w_down, ((128, BF), (128, BF)))
    sum_far = moved(far_part, "tensor", 2)
    sum_one = moved(for_right, "tensor", 1)
    sum_two = moved(for_left, "tensor", -1)
    block = lambda n: pl.BlockSpec((n, D), lambda i: (i, 0))
    hidden = call(
        final_body, shape((QT, D)), [after, own_part, sum_one, sum_two, sum_far], grid=(2,),
        in_specs=[block(64)] * 5, out_specs=block(64), flops=1 << 20, size=3 << 20, limit=8 << 20,
    )

    totals = call(
        totals_body, shape((2, D), F32), [near_sums, far_sums, own_sums, after_sum], flops=1 << 16, size=1 << 19, limit=4 << 20,
    )
    rest = [moved(totals, "tensor", s) for s in (1, -1, 2)]
    totals = call(sum_body, shape((2, D), F32), [totals, *rest], flops=1 << 14, size=1 << 17, limit=4 << 20)
    rest = [moved(totals, "x", s) for s in (1, -1, 2)]
    over_x = call(stack_body, shape((4, 2, D), F32), [totals, *rest], flops=1 << 14, size=1 << 17, limit=4 << 20)
    below, above, across = (moved(over_x, "y", s) for s in (1, -1, 2))
    values = call(
        states_body,
        shape((FRAMES, HD), F32),
        [valid_frames, over_x, above, below, across, line(pool_gain), line(pool_bias), line(value_weight)],
        [pltpu.VMEM((16, 2, D), F32), pltpu.VMEM((FRAMES, D), F32)],
        in_specs=[pl.BlockSpec(memory_space=SMEM)] + [pl.BlockSpec(memory_space=VMEM)] * 7,
        flops=1 << 20,
        size=1 << 20,
        limit=8 << 20,
    )
    other_values = lax.ppermute(values, "dp", swap)
    frame_values, advantages = call(
        advantages_body,
        [shape((1, 2), F32)] * 2,
        [valid_frames, values, other_values],
        in_specs=[pl.BlockSpec(memory_space=SMEM)] + [pl.BlockSpec(memory_space=VMEM)] * 2,
        flops=1 << 14,
        size=1 << 15,
        limit=4 << 20,
    )
    return hidden[None], frame_values, advantages


def solution(mesh):
    fine = Mesh(mesh.devices.reshape(2, 4, 4, 4), ("dp", "y", "x", "tensor"))
    token_spec = P("dp", ("y", "x", "tensor"), None)
    in_specs = (
        token_spec,
        P(),
        P(None, None, "tensor"),
        P("tensor", None),
        P(),
        P(None, "tensor"),
        P("tensor", None),
        P(),
        P(),
        P(),
        P(),
    )
    out_specs = (token_spec, P("dp", ("y", "x")), P("dp", ("y", "x")))
    return jax.shard_map(local, mesh=fine, in_specs=in_specs, out_specs=out_specs, check_vma=False)
```

```python
import functools
import math

import jax
import jax.numpy as jnp
from jax import lax
from jax.experimental import pallas as pl
from jax.experimental.pallas import tpu as pltpu
from jax.sharding import Mesh, PartitionSpec as P


D = 2048
HD = 128
QT = 128
FRAMES = 32
TOK_FRAME = 256
BF = jnp.bfloat16
F32 = jnp.float32
QSCALE = math.log2(math.e) / math.sqrt(HD)
SHIFTS = (0, -1, 1, 2)
QKV_LIMIT = 12 << 20
PROJECT_LIMIT = 12 << 20
MLP_LIMIT = 12 << 20
VMEM = pltpu.VMEM
SMEM = pltpu.SMEM


def ring(shift):
    return [(i, (i + shift) % 4) for i in range(4)]


def moved(array, axis, shift):
    return lax.ppermute(array, axis, ring(shift))


def flat(*digits):
    sizes = {2: (2, 4), 3: (2, 4, 4)}[len(digits)]
    at = 0
    for digit, size in zip(digits, sizes):
        at = at * size + digit
    return at


def seats():
    return tuple(lax.axis_index(name).astype(jnp.int32) for name in ("dp", "y", "x", "tensor"))


def call(body, out, ins, scratch=(), grid=None, in_specs=None, out_specs=None, flops=0, size=0, limit=None):
    single = not isinstance(out, (list, tuple))
    outs = [out] if single else list(out)
    whole = pl.BlockSpec(memory_space=VMEM)
    kwargs = {} if grid is None else {"grid": grid}
    return pl.pallas_call(
        body,
        out_shape=out if single else outs,
        in_specs=in_specs or [whole] * len(ins),
        out_specs=out_specs or (whole if single else [whole] * len(outs)),
        scratch_shapes=list(scratch),
        compiler_params=pltpu.CompilerParams(vmem_limit_bytes=limit),
        cost_estimate=pl.CostEstimate(flops=flops, bytes_accessed=size, transcendentals=0),
        **kwargs,
    )(*ins)


def shape(dims, kind=BF):
    return jax.ShapeDtypeStruct(tuple(dims), kind)


def normalized(floats, gain):
    square = jnp.mean(floats * floats, axis=-1, keepdims=True)
    return (floats * lax.rsqrt(square + 1e-05) * gain).astype(BF)


def qkv_body(parts, gain, *refs):
    rows, w, outs, normed, made = refs[:parts], refs[parts], refs[parts + 1 : parts + 5], refs[-2], refs[-1]
    x = seats()[2]
    at = 0
    for part in rows:
        n = part.shape[0]
        normed[at : at + n, :] = normalized(part[...].astype(F32), gain[...])
        at += n

    def step(c, carry):
        product = jnp.dot(normed[...], w[c], preferred_element_type=F32)
        product = product * jnp.where(c == 0, QSCALE, 1.0)
        made[...] = product.astype(BF)
        slot = lax.rem(c + 2, 3)
        for rel in range(4):
            head = lax.rem(x + rel, 4)
            outs[rel][:, pl.ds(pl.multiple_of(slot * HD, HD), HD)] = made[:, pl.ds(pl.multiple_of(head * HD, HD), HD)]
        return carry

    lax.fori_loop(0, 3, step, 0)


def qkv_of(gain, parts, w):
    n = sum(part.shape[0] for part in parts)
    return call(
        functools.partial(qkv_body, len(parts)),
        [shape((n, 3 * HD))] * 4,
        [gain, *parts, w],
        [pltpu.VMEM((n, D), BF), pltpu.VMEM((n, 4 * HD), BF)],
        flops=2 * n * D * 12 * HD,
        size=7 << 20,
        limit=QKV_LIMIT,
    )


def attention_body(spread, first, lengths, *refs):
    qs, mine, theirs = refs[:4], refs[4], refs[5]
    given, outs = ((), refs[6:8]) if first else (refs[6:8], refs[8:12])
    q_all, k_all, v_all, held, tops_all, sem = refs[-6:]
    c, y, x, z = seats()
    quarter = 2 * lax.rem(y, 2) + c
    roll = lax.div(y, 2)
    length = lengths[roll]
    home = c == roll
    xs = [lax.rem(x + 4 + s, 4) for s in SHIFTS]
    twin = (lambda v: v) if first else (lambda v: v + 1 - 2 * lax.rem(v, 2))
    one, two = twin(jnp.where(home, y, 3 - y)), twin(jnp.where(home, 3 - y, y))

    def copies(act):
        for k in range(4):
            source = lax.rem(quarter + 4 - k, 4)
            for i in range(4):
                act(pltpu.make_async_copy(qs[k].at[i], q_all.at[source * 4 + xs[i]], sem))
        for slot, array in enumerate((mine, theirs)):
            for i in range(4):
                for p, shift in enumerate(spread):
                    at = (slot * 16 + xs[i] * 4 + lax.rem(z + 4 + shift, 4)) * QT
                    at = pl.ds(pl.multiple_of(at, QT), QT)
                    rows = pl.ds(p * QT, QT)
                    act(pltpu.make_async_copy(array.at[i, rows, pl.ds(0, HD)], k_all.at[at, :], sem))
                    act(pltpu.make_async_copy(array.at[i, rows, pl.ds(HD, HD)], v_all.at[at, pl.ds(0, HD)], sem))

    copies(lambda copy: copy.start())
    v_all[:, HD:] = jnp.ones((4096, HD), BF)
    if first:
        acc, peak = outs
        acc[...] = jnp.zeros((2048, 2 * HD), F32)
        peak[...] = jnp.full((2048, HD), -1e30, F32)
    else:
        acc, peak = refs[-8:-6]
        acc[...] = given[0][...]
        peak[...] = given[1][...]
    copies(lambda copy: copy.wait())

    high = lax.shift_right_logical(quarter, 1)
    blocks_in = lax.div(length + 7, 8)
    parts = [slice(rb * QT, (rb + 1) * QT) for rb in range(4)]
    count_one = jnp.where(one < blocks_in, 4 - one, 0)
    count = count_one + jnp.where(two < blocks_in, 4 - two, 0)

    def pair_at(p):
        slot = jnp.where(p >= count_one, 1, 0)
        block = jnp.where(p >= count_one, two, one)
        return slot, block, block + p - slot * count_one

    def bias(block, Y, kb, rb, half):
        seen = 2 * (block * 4 + kb) + half
        return jnp.where((seen <= 2 * (4 * Y + rb) + high) & (seen < length), 0.0, -1e30).astype(F32)

    def keys_at(slot, kb):
        return pl.ds(pl.multiple_of((slot * 4 + kb) * 512, 512), 512)

    def score(pair, kb, tops):
        slot, block, Y = pair
        q = q_all[pl.ds(Y * 4, 4)].reshape(512, HD)
        s = lax.dot_general(q, k_all[keys_at(slot, kb), :], (((1,), (1,)), ((), ())), preferred_element_type=F32)
        held[kb] = s
        made = []
        for rb in range(4):
            top = tops[rb]
            for half in range(2):
                piece = s[parts[rb], half * TOK_FRAME : (half + 1) * TOK_FRAME]
                top = jnp.maximum(top, jnp.maximum(piece[:, :HD], piece[:, HD:]) + bias(block, Y, kb, rb, half))
            made.append(top)
        return made

    def keep(tops):
        for rb in range(4):
            tops_all[parts[rb], :] = jnp.broadcast_to(jnp.max(tops[rb], axis=1, keepdims=True), (QT, HD))

    lowest = [jnp.full((QT, HD), -1e30, F32)] * 4
    tops = lowest
    for kb in range(4):
        tops = score(pair_at(0), kb, tops)
    keep(tops)

    def step(p, carry):
        slot, block, Y = pair_at(p)
        following = pair_at(jnp.minimum(p + 1, count - 1))
        rows_in = pl.ds(pl.multiple_of(Y * 512, 512), 512)
        before = peak[rows_in, :]
        now = jnp.maximum(before, tops_all[...])
        total = acc[rows_in, :] * jnp.exp2(before - now)[:, :1]
        peak[rows_in, :] = now
        tops = lowest
        for kb in range(4):
            rows = []
            for rb in range(4):
                row = [
                    jnp.exp2(held[kb, parts[rb], half * TOK_FRAME : (half + 1) * TOK_FRAME]
                             - (now[parts[rb], :1] - bias(block, Y, kb, rb, half))).astype(BF)
                    for half in range(2)
                ]
                rows.append(jnp.concatenate(row, axis=1))
            weights = jnp.concatenate(rows, axis=0)
            total = total + jnp.dot(weights, v_all[keys_at(slot, kb), :], preferred_element_type=F32)
            tops = score(following, kb, tops)
        acc[rows_in, :] = total
        keep(tops)
        return carry

    lax.fori_loop(0, count, step, 0)
    if first:
        return
    for k in range(4):
        source = lax.rem(quarter + 4 - k, 4)
        for i in range(4):
            at = pl.multiple_of((source * 4 + xs[i]) * QT, QT)
            rows_in = pl.ds(at, QT)
            outs[i][k] = (acc[rows_in, :HD] / acc[rows_in, HD:]).astype(BF)


def attention(lengths, qs, mine, theirs, spread, given=()):
    first = not given
    anyspace = pl.BlockSpec(memory_space=pl.ANY)
    whole = pl.BlockSpec(memory_space=VMEM)
    state = [shape((2048, 2 * HD), F32), shape((2048, HD), F32)]
    working = [] if first else [pltpu.VMEM((2048, 2 * HD), F32), pltpu.VMEM((2048, HD), F32)]
    outs = state if first else [shape((4, QT, HD))] * 4
    return call(
        functools.partial(attention_body, spread, first),
        outs,
        [lengths, *qs, mine, theirs, *given],
        [
            *working,
            pltpu.VMEM((16, QT, HD), BF),
            pltpu.VMEM((4096, HD), BF),
            pltpu.VMEM((4096, 2 * HD), BF),
            pltpu.VMEM((4, 512, 512), F32),
            pltpu.VMEM((512, HD), F32),
            pltpu.SemaphoreType.DMA,
        ],
        in_specs=[pl.BlockSpec(memory_space=SMEM)] + [anyspace] * 6 + [whole] * len(given),
        out_specs=[whole] * len(outs),
        flops=3 << 30,
        size=8 << 20,
        limit=24 << 20,
    )


def project_body(gain, rows, *refs):
    mixed_in, ws = refs[:4], refs[4:9]
    after, top, low, total, mixed, acc = refs[9:]
    c, y, x, z = seats()
    for kk in range(4):
        z_from = lax.rem(y + 4 - kk, 4)
        for i, s in enumerate(SHIFTS):
            head = z_from * 4 + lax.rem(x + 4 - s, 4)
            mixed[:, pl.ds(pl.multiple_of(head * HD, HD), HD)] = mixed_in[kk][i]

    def step(n, carry):
        columns = pl.ds(pl.multiple_of(n * 512, 512), 512)

        def term(slab, offset, w):
            at = pl.multiple_of(lax.rem(slab, 4) * 512 + offset, 256)
            return jnp.dot(mixed[:, pl.ds(at, w.shape[0])], w[:, columns], preferred_element_type=F32)

        sums = term(z, 0, ws[0])
        sums = sums + term(z + 3 + 2 * c, 0, ws[1]) + term(z + 5 - 2 * c, 0, ws[2])
        sums = sums + term(z + 2, c * 256, ws[3]) + term(z + 2, (1 - c) * 256, ws[4])
        acc[:, columns] = sums
        return carry

    lax.fori_loop(0, 4, step, 0)
    rounded = (rows[...].astype(F32) + acc[...]).astype(BF)
    after[...] = rounded
    floats = rounded.astype(F32)
    normed2 = normalized(floats, gain[...])
    top[...] = normed2[: QT // 2]
    low[...] = normed2[QT // 2 :]
    total[...] = jnp.broadcast_to(jnp.sum(floats, axis=0, keepdims=True), (8, D))


def project(gain, rows, mixed_in, ws):
    return call(
        project_body,
        [shape((QT, D)), shape((QT // 2, D)), shape((QT // 2, D)), shape((8, D), F32)],
        [gain, rows, *mixed_in, *ws],
        [pltpu.VMEM((QT, D), BF), pltpu.VMEM((QT, D), F32)],
        flops=2 * QT * D * D,
        size=9 << 20,
        limit=PROJECT_LIMIT,
    )


def pack_body(*refs):
    out = refs[4]
    for i in range(4):
        out[i] = refs[i][...]


def pack(pieces):
    n = pieces[0].shape[0]
    return call(
        pack_body, shape((4, n, 2 * HD)), pieces, grid=(1,),
        in_specs=[pl.BlockSpec((n, 2 * HD), lambda i: (0, 0))] * 4,
        out_specs=pl.BlockSpec((4, n, 2 * HD), lambda i: (0, 0, 0)),
        flops=1 << 22, size=n << 12, limit=8 << 20,
    )


def share_body(*refs):
    out = refs[6]
    home = seats()[0] == lax.div(seats()[1], 2)
    for pick, when in ((0, home), (1, jnp.logical_not(home))):

        @pl.when(when)
        def _():
            at = 0
            for g in range(3):
                part = refs[2 * g + pick]
                out[:, at : at + part.shape[1], :] = part[...]
                at += part.shape[1]


def final_body(after, own, *refs):
    total = after[...].astype(F32) + own[...]
    for part in refs[:3]:
        total = total + part[...].astype(F32)
    refs[3][...] = total.astype(BF)


def queries_body(order, *refs):
    pieces, outs = refs[:12], refs[12:]
    _, y, _, z = seats()
    for k in range(4):
        turn = lax.rem(y + k + 4 - z, 4)
        for shift in range(4):
            group, part = order[shift]

            @pl.when(turn == shift)
            def _():
                for i in range(4):
                    outs[k][i] = pieces[group * 4 + i][part * QT : (part + 1) * QT, :]


def queries(groups, order):
    pieces = [piece for group in groups for piece in group]
    return call(
        functools.partial(queries_body, order), [shape((4, QT, HD))] * 4, pieces, grid=(1,),
        in_specs=[pl.BlockSpec((p.shape[0], HD), lambda i: (0, 2)) for p in pieces],
        out_specs=[pl.BlockSpec((4, QT, HD), lambda i: (0, 0, 0))] * 4,
        flops=1 << 22, size=1 << 20, limit=8 << 20,
    )


def heads_body(*refs):
    c, y, _, z = seats()
    quarter = 2 * lax.rem(y, 2) + c
    for kk in range(4):
        k = lax.rem(quarter + 8 - z - kk, 4)
        for i in range(4):
            refs[4 + kk][i] = refs[i][k]


def mlp_body(parts, cuts, *refs):
    rows, w_up, w_down = refs[:parts], refs[parts], refs[parts + 1]
    outs = refs[-4 - len(cuts) : -4]
    sums, inside, upper, acc = refs[-4:]
    n, block = inside.shape[0], upper.shape[1]
    at = 0
    for part in rows:
        inside[at : at + part.shape[0], :] = part[...]
        at += part.shape[0]
    acc[...] = jnp.zeros_like(acc)
    index = lax.broadcasted_iota(jnp.int32, (16, block), 0)

    def step(f, carry):
        span = pl.ds(pl.multiple_of(f * block, block), block)
        hidden = jnp.dot(inside[...], w_up[:, span], preferred_element_type=F32)
        up = jax.nn.gelu(hidden, approximate=True).astype(BF)
        upper[:n, :] = up
        extra = jnp.zeros((16, block), F32)
        for q in range(n // QT):
            whole = jnp.sum(up[q * QT : (q + 1) * QT, :].astype(F32), axis=0, keepdims=True)
            high = whole.astype(BF).astype(F32)
            extra = jnp.where(index == 2 * q, high, jnp.where(index == 2 * q + 1, whole - high, extra))
        upper[n:, :] = extra.astype(BF)
        acc[...] += jnp.dot(upper[...], w_down[span, :], preferred_element_type=F32)
        return carry

    lax.fori_loop(0, w_up.shape[1] // block, step, 0)
    at = 0
    for out in outs:
        out[...] = acc[at : at + out.shape[0], :].astype(out.dtype)
        at += out.shape[0]
    sums[...] = acc[n:, :]


def mlp(parts, w_up, w_down, cuts):
    n = sum(part.shape[0] for part in parts)
    return call(
        functools.partial(mlp_body, len(parts), cuts),
        [*(shape((size, D), kind) for size, kind in cuts), shape((16, D), F32)],
        [*parts, w_up, w_down],
        [pltpu.VMEM((n, D), BF), pltpu.VMEM((n + 16, 512), BF), pltpu.VMEM((n + 16, D), F32)],
        flops=4 * n * D * w_up.shape[1],
        size=17 << 20,
        limit=MLP_LIMIT,
    )


def half_body(w, out, sem):
    rows = pl.ds(pl.multiple_of(lax.axis_index("dp").astype(jnp.int32) * 256, 256), 256)
    copy = pltpu.make_async_copy(w.at[rows, :], out, sem)
    copy.start()
    copy.wait()


def totals_body(near, far, mine, after, out):
    z = seats()[3]
    own = mine[0:1, :] + mine[1:2, :] + after[0:1, :]
    parts = ((0, own), (3, near[0:1, :] + near[1:2, :]), (1, near[2:3, :] + near[3:4, :]), (2, far[0:1, :] + far[1:2, :]))
    for frame in range(2):
        total = jnp.zeros((1, D), F32)
        for shift, part in parts:
            total = total + part * jnp.where(lax.rem(z + shift, 4) // 2 == frame, 1.0, 0.0)
        out[frame : frame + 1, :] = total


def stack_body(*refs):
    for i in range(4):
        refs[4][i] = refs[i][...]


def sum_body(*refs):
    refs[4][...] = refs[0][...] + refs[1][...] + refs[2][...] + refs[3][...]


def both_body(one, two, out):
    out[:2, :] = one[...]
    out[2:, :] = two[...]


def states_body(lengths, near, above, below, far, gain, bias, weight, *refs):
    means, states = refs[2:]
    c, y, x, _ = seats()
    for array, ys in ((near, 0), (below, -1), (above, 1), (far, 2)):
        for i, s in enumerate(SHIFTS):
            at = lax.rem(y + 4 + ys, 4) * 4 + lax.rem(x + 4 + s, 4)
            means[at] = array[i] * (1.0 / TOK_FRAME)
    index = lax.broadcasted_iota(jnp.int32, (FRAMES, HD), 0)
    for roll in range(2):
        length = lengths[c if roll == 0 else 1 - c]
        state = jnp.zeros((1, D), F32)
        for frame in range(FRAMES):
            row = 2 * roll + frame % 2
            mean = means[frame // 2, row : row + 1, :]
            gate = jax.nn.sigmoid(mean * gain[...] + bias[...])
            state = jnp.where(frame < length, gate * state + (1.0 - gate) * mean, state)
            states[frame : frame + 1, :] = state
        values = jnp.sum(states[...] * weight[...], axis=1, keepdims=True)
        refs[roll][...] = jnp.where(index < length, values, 0.0)


def advantages_body(lengths, mine, theirs, out):
    c, y, x, _ = seats()
    index = lax.broadcasted_iota(jnp.int32, (FRAMES, HD), 0)
    lane = lax.broadcasted_iota(jnp.int32, (1, HD), 1)
    summed = lambda v: jnp.sum(v, axis=0, keepdims=True)
    at = (y * 4 + x) * 2
    values = (mine[...], theirs[...])
    sizes = (lengths[c], lengths[1 - c])
    gaps = []
    for value, size in zip(values, sizes):
        final = summed(jnp.where(index == size - 1, value, 0.0))
        gaps.append(jnp.where(index < size, final - value, 0.0))
    count = (sizes[0] + sizes[1]).astype(F32)
    mean = (summed(gaps[0]) + summed(gaps[1])) / count
    centered = [jnp.where(index < size, gap - mean, 0.0) for gap, size in zip(gaps, sizes)]
    variance = (summed(centered[0] * centered[0]) + summed(centered[1] * centered[1])) / count
    out[...] = jnp.zeros((8, HD), F32)
    for roll in range(2):
        scaled = jnp.where(index < sizes[roll], centered[roll] * lax.rsqrt(variance + 1e-05), 0.0)
        for kind, array in enumerate((values[roll], scaled)):
            one, two = (summed(jnp.where(index == at + e, array, 0.0)) for e in (0, 1))
            row = 2 * roll + kind
            out[row : row + 1, :] = jnp.where(lane == 0, one, two)


def pick_body(made, given, first, second):
    owner = lax.axis_index("dp") == 1
    for kind, out in enumerate((first, second)):
        out[...] = jnp.where(owner, made[kind : kind + 1, :2], given[2 + kind : 3 + kind, :2])


def local(tokens, attn_gain, w_qkv, w_out, mlp_gain, w_up, w_down, pool_gain, pool_bias, value_weight, valid_frames):
    rows = tokens[0]
    line = lambda v: v.reshape(1, D)

    from_left = moved(rows, "tensor", 1)
    from_right = moved(rows, "tensor", -1)
    far_top = moved(from_left[:64], "tensor", 1)
    far_low = moved(from_right[64:], "tensor", -1)
    groups = (((rows,), (0,)), ((from_left, from_right), (-1, 1)), ((far_top, far_low), (2,)))
    spread = tuple(shift for group in groups for shift in group[1])

    pa_pairs, pb_pairs = [], []
    for core in range(2):
        for yy in range(4):
            if yy // 2 == core:
                pa_pairs.append((flat(core, yy), flat(core, yy ^ 1)))
            else:
                pa_pairs.append((flat(core, yy), flat(1 - core, 3 - yy)))
                pb_pairs.append((flat(core, yy), flat(core, yy ^ 1)))
    swap = [(0, 1), (1, 0)]

    chunks, held, order = [], [], {}
    for g, (parts, shifts) in enumerate(groups):
        made = qkv_of(line(attn_gain), parts, w_qkv)
        got = [made[0], moved(made[1], "x", 1), moved(made[3], "x", -1), moved(made[2], "x", 2)]
        held.append(got)
        block = pack(got)
        pa = lax.ppermute(block, ("dp", "y"), pa_pairs)
        pb = lax.ppermute(pa, ("dp", "y"), pb_pairs)
        chunks.append((block, pa, pb))
        for p, shift in enumerate(shifts):
            order[shift % 4] = (g, p)
    qs = []
    for k, part in enumerate(queries(held, order)):
        pairs = []
        for core in range(2):
            for yy in range(4):
                j = (yy + k) % 4
                pairs.append((flat(core, yy), flat(j % 2, 2 * core + j // 2)))
        qs.append(lax.ppermute(part, ("dp", "y"), pairs))

    shared = []
    for b in range(2):
        mine = call(
            share_body, shape((4, 512, 2 * HD)), [chunk[b + i] for chunk in chunks for i in range(2)],
            flops=1 << 24, size=2 << 20, limit=10 << 20,
        )
        shared.append((mine, lax.ppermute(mine, "dp", swap)))
    state = attention(valid_frames, qs, *shared[0], spread)
    outs = attention(valid_frames, qs, *shared[1], spread, tuple(state))

    w_first, _, _ = lax.optimization_barrier((w_out, far_low, far_top))
    pairs = [(4 * core + zz, 4 * core + (zz + 1 - 2 * core) % 4) for core in range(2) for zz in range(4)]
    w_near = lax.ppermute(w_first, ("dp", "tensor"), pairs)
    w_half = call(
        half_body, shape((256, D)), [w_near], [pltpu.SemaphoreType.DMA],
        in_specs=[pl.BlockSpec(memory_space=pl.ANY)], flops=1 << 22, size=2 << 20, limit=4 << 20,
    )
    w_far = lax.ppermute(w_half, ("dp", "tensor"), pairs)
    ws = [w_out, w_near, lax.ppermute(w_near, "dp", swap), w_far, lax.ppermute(w_far, "dp", swap)]

    heads = [outs[0], moved(outs[1], "x", -1), moved(outs[2], "x", 1), moved(outs[3], "x", 2)]
    heads = call(heads_body, [shape((4, QT, HD))] * 4, heads, flops=1 << 22, size=1 << 20, limit=8 << 20)
    mixed_in = []
    for kk, part in enumerate(heads):
        pairs = []
        for core in range(2):
            for yy in range(4):
                for zz in range(4):
                    j = 2 * (yy % 2) + core
                    pairs.append((flat(core, yy, zz), flat(yy // 2, (zz + kk) % 4, j)))
        mixed_in.append(lax.ppermute(part, ("dp", "y", "tensor"), pairs))
    after, top, low, after_sum = project(line(mlp_gain), rows, mixed_in, ws)

    left_top = moved(top, "tensor", 1)
    right_low = moved(low, "tensor", -1)
    opposite_top = moved(left_top, "tensor", 1)
    opposite_low = moved(right_low, "tensor", -1)
    left_low = moved(low, "tensor", 1)
    right_top = moved(top, "tensor", -1)
    own_part, own_sums = mlp((top, low), w_up, w_down, ((128, F32),))
    far_part, far_sums = mlp((opposite_top, opposite_low), w_up, w_down, ((128, BF),))
    near_in = (left_top, left_low, right_top, right_low)
    for_left, for_right, near_sums = mlp(near_in, w_up, w_down, ((128, BF), (128, BF)))
    sum_far = moved(far_part, "tensor", 2)
    sum_one = moved(for_right, "tensor", 1)
    sum_two = moved(for_left, "tensor", -1)
    block = lambda n: pl.BlockSpec((n, D), lambda i: (i, 0))
    hidden = call(
        final_body, shape((QT, D)), [after, own_part, sum_one, sum_two, sum_far], grid=(2,),
        in_specs=[block(64)] * 5, out_specs=block(64), flops=1 << 20, size=3 << 20, limit=8 << 20,
    )

    totals = call(
        totals_body, shape((2, D), F32), [near_sums, far_sums, own_sums, after_sum], flops=1 << 16, size=1 << 19, limit=4 << 20,
    )
    over = lambda array, axis, shift: lax.ppermute(
        array, ("dp", axis), [(4 + i, 4 + (i + shift) % 4) for i in range(4)]
    )
    theirs = lax.ppermute(totals, "dp", [(0, 1)])
    totals = call(both_body, shape((4, D), F32), [totals, theirs], flops=1 << 14, size=1 << 17, limit=4 << 20)
    rest = [over(totals, "tensor", s) for s in (1, -1, 2)]
    totals = call(sum_body, shape((4, D), F32), [totals, *rest], flops=1 << 14, size=1 << 17, limit=4 << 20)
    rest = [over(totals, "x", s) for s in (1, -1, 2)]
    over_x = call(stack_body, shape((4, 4, D), F32), [totals, *rest], flops=1 << 14, size=1 << 17, limit=4 << 20)
    below, above, across = (over(over_x, "y", s) for s in (1, -1, 2))
    smem, vmem = pl.BlockSpec(memory_space=SMEM), pl.BlockSpec(memory_space=VMEM)
    values = call(
        states_body,
        [shape((FRAMES, HD), F32)] * 2,
        [valid_frames, over_x, above, below, across, line(pool_gain), line(pool_bias), line(value_weight)],
        [pltpu.VMEM((16, 4, D), F32), pltpu.VMEM((FRAMES, D), F32)],
        in_specs=[smem] + [vmem] * 7,
        flops=1 << 20,
        size=1 << 20,
        limit=8 << 20,
    )
    made = call(
        advantages_body,
        shape((8, HD), F32),
        [valid_frames, *values],
        in_specs=[smem] + [vmem] * 2,
        flops=1 << 14,
        size=1 << 15,
        limit=4 << 20,
    )
    given = lax.ppermute(made, "dp", [(1, 0)])
    frame_values, advantages = call(
        pick_body, [shape((1, 2), F32)] * 2, [made, given], flops=1 << 10, size=1 << 13, limit=4 << 20,
    )
    return hidden[None], frame_values, advantages


def solution(mesh):
    fine = Mesh(mesh.devices.reshape(2, 4, 4, 4), ("dp", "y", "x", "tensor"))
    token_spec = P("dp", ("y", "x", "tensor"), None)
    in_specs = (
        token_spec,
        P(),
        P(None, None, "tensor"),
        P("tensor", None),
        P(),
        P(None, "tensor"),
        P("tensor", None),
        P(),
        P(),
        P(),
        P(),
    )
    out_specs = (token_spec, P("dp", ("y", "x")), P("dp", ("y", "x")))
    return jax.shard_map(local, mesh=fine, in_specs=in_specs, out_specs=out_specs, check_vma=False)
```

```python
import functools
import math

import jax
import jax.numpy as jnp
from jax import lax
from jax.experimental import pallas as pl
from jax.experimental.pallas import tpu as pltpu
from jax.sharding import Mesh, PartitionSpec as P


D = 2048
HD = 128
QT = 128
FRAMES = 32
TOK_FRAME = 256
BF = jnp.bfloat16
F32 = jnp.float32
QSCALE = math.log2(math.e) / math.sqrt(HD)
SHIFTS = (0, -1, 1, 2)
QKV_LIMIT = 12 << 20
PROJECT_LIMIT = 12 << 20
MLP_LIMIT = 12 << 20
VMEM = pltpu.VMEM
SMEM = pltpu.SMEM


def ring(shift):
    return [(i, (i + shift) % 4) for i in range(4)]


def moved(array, axis, shift):
    return lax.ppermute(array, axis, ring(shift))


def flat(*digits):
    sizes = {2: (2, 4), 3: (2, 4, 4)}[len(digits)]
    at = 0
    for digit, size in zip(digits, sizes):
        at = at * size + digit
    return at


def seats():
    return tuple(lax.axis_index(name).astype(jnp.int32) for name in ("dp", "y", "x", "tensor"))


def call(body, out, ins, scratch=(), grid=None, in_specs=None, out_specs=None, flops=0, size=0, limit=None):
    single = not isinstance(out, (list, tuple))
    outs = [out] if single else list(out)
    whole = pl.BlockSpec(memory_space=VMEM)
    kwargs = {} if grid is None else {"grid": grid}
    return pl.pallas_call(
        body,
        out_shape=out if single else outs,
        in_specs=in_specs or [whole] * len(ins),
        out_specs=out_specs or (whole if single else [whole] * len(outs)),
        scratch_shapes=list(scratch),
        compiler_params=pltpu.CompilerParams(vmem_limit_bytes=limit),
        cost_estimate=pl.CostEstimate(flops=flops, bytes_accessed=size, transcendentals=0),
        **kwargs,
    )(*ins)


def shape(dims, kind=BF):
    return jax.ShapeDtypeStruct(tuple(dims), kind)


def normalized(floats, gain):
    square = jnp.mean(floats * floats, axis=-1, keepdims=True)
    return (floats * lax.rsqrt(square + 1e-05) * gain).astype(BF)


def qkv_body(parts, gain, *refs):
    rows, w, outs, normed, made = refs[:parts], refs[parts], refs[parts + 1 : parts + 5], refs[-2], refs[-1]
    x = seats()[2]
    at = 0
    for part in rows:
        n = part.shape[0]
        normed[at : at + n, :] = normalized(part[...].astype(F32), gain[...])
        at += n

    def step(c, carry):
        product = jnp.dot(normed[...], w[c], preferred_element_type=F32)
        product = product * jnp.where(c == 0, QSCALE, 1.0)
        made[...] = product.astype(BF)
        slot = lax.rem(c + 2, 3)
        for rel in range(4):
            head = lax.rem(x + rel, 4)
            outs[rel][:, pl.ds(pl.multiple_of(slot * HD, HD), HD)] = made[:, pl.ds(pl.multiple_of(head * HD, HD), HD)]
        return carry

    lax.fori_loop(0, 3, step, 0)


def qkv_of(gain, parts, w):
    n = sum(part.shape[0] for part in parts)
    return call(
        functools.partial(qkv_body, len(parts)),
        [shape((n, 3 * HD))] * 4,
        [gain, *parts, w],
        [pltpu.VMEM((n, D), BF), pltpu.VMEM((n, 4 * HD), BF)],
        flops=2 * n * D * 12 * HD,
        size=7 << 20,
        limit=QKV_LIMIT,
    )


def attention_body(spread, first, lengths, *refs):
    qs, mine, theirs = refs[:4], refs[4], refs[5]
    given, outs = ((), refs[6:8]) if first else (refs[6:8], refs[8:12])
    q_all, k_all, v_all, held, tops_all, sem = refs[-6:]
    c, y, x, z = seats()
    quarter = 2 * lax.rem(y, 2) + c
    roll = lax.div(y, 2)
    length = lengths[roll]
    home = c == roll
    xs = [lax.rem(x + 4 + s, 4) for s in SHIFTS]
    twin = (lambda v: v) if first else (lambda v: v + 1 - 2 * lax.rem(v, 2))
    one, two = twin(jnp.where(home, y, 3 - y)), twin(jnp.where(home, 3 - y, y))

    def copies(act):
        for k in range(4):
            source = lax.rem(quarter + 4 - k, 4)
            for i in range(4):
                act(pltpu.make_async_copy(qs[k].at[i], q_all.at[source * 4 + xs[i]], sem))
        for slot, array in enumerate((mine, theirs)):
            for i in range(4):
                for p, shift in enumerate(spread):
                    at = (slot * 16 + xs[i] * 4 + lax.rem(z + 4 + shift, 4)) * QT
                    at = pl.ds(pl.multiple_of(at, QT), QT)
                    rows = pl.ds(p * QT, QT)
                    act(pltpu.make_async_copy(array.at[i, rows, pl.ds(0, HD)], k_all.at[at, :], sem))
                    act(pltpu.make_async_copy(array.at[i, rows, pl.ds(HD, HD)], v_all.at[at, pl.ds(0, HD)], sem))

    copies(lambda copy: copy.start())
    v_all[:, HD:] = jnp.ones((4096, HD), BF)
    if first:
        acc, peak = outs
        acc[...] = jnp.zeros((2048, 2 * HD), F32)
        peak[...] = jnp.full((2048, HD), -1e30, F32)
    else:
        acc, peak = refs[-8:-6]
        acc[...] = given[0][...]
        peak[...] = given[1][...]
    copies(lambda copy: copy.wait())

    high = lax.shift_right_logical(quarter, 1)
    blocks_in = lax.div(length + 7, 8)
    parts = [slice(rb * QT, (rb + 1) * QT) for rb in range(4)]
    count_one = jnp.where(one < blocks_in, 4 - one, 0)
    count = count_one + jnp.where(two < blocks_in, 4 - two, 0)

    def pair_at(p):
        slot = jnp.where(p >= count_one, 1, 0)
        block = jnp.where(p >= count_one, two, one)
        return slot, block, block + p - slot * count_one

    def bias(block, Y, kb, rb, half):
        seen = 2 * (block * 4 + kb) + half
        return jnp.where((seen <= 2 * (4 * Y + rb) + high) & (seen < length), 0.0, -1e30).astype(F32)

    def keys_at(slot, kb):
        return pl.ds(pl.multiple_of((slot * 4 + kb) * 512, 512), 512)

    def score(pair, kb, tops):
        slot, block, Y = pair
        q = q_all[pl.ds(Y * 4, 4)].reshape(512, HD)
        s = lax.dot_general(q, k_all[keys_at(slot, kb), :], (((1,), (1,)), ((), ())), preferred_element_type=F32)
        held[kb] = s
        made = []
        for rb in range(4):
            top = tops[rb]
            for half in range(2):
                piece = s[parts[rb], half * TOK_FRAME : (half + 1) * TOK_FRAME]
                top = jnp.maximum(top, jnp.maximum(piece[:, :HD], piece[:, HD:]) + bias(block, Y, kb, rb, half))
            made.append(top)
        return made

    def keep(tops):
        for rb in range(4):
            tops_all[parts[rb], :] = jnp.broadcast_to(jnp.max(tops[rb], axis=1, keepdims=True), (QT, HD))

    lowest = [jnp.full((QT, HD), -1e30, F32)] * 4
    tops = lowest
    for kb in range(4):
        tops = score(pair_at(0), kb, tops)
    keep(tops)

    def step(p, carry):
        slot, block, Y = pair_at(p)
        following = pair_at(jnp.minimum(p + 1, count - 1))
        rows_in = pl.ds(pl.multiple_of(Y * 512, 512), 512)
        before = peak[rows_in, :]
        now = jnp.maximum(before, tops_all[...])
        total = acc[rows_in, :] * jnp.exp2(before - now)[:, :1]
        peak[rows_in, :] = now
        tops = lowest
        for kb in range(4):
            rows = []
            for rb in range(4):
                row = [
                    jnp.exp2(held[kb, parts[rb], half * TOK_FRAME : (half + 1) * TOK_FRAME]
                             - (now[parts[rb], :1] - bias(block, Y, kb, rb, half))).astype(BF)
                    for half in range(2)
                ]
                rows.append(jnp.concatenate(row, axis=1))
            weights = jnp.concatenate(rows, axis=0)
            total = total + jnp.dot(weights, v_all[keys_at(slot, kb), :], preferred_element_type=F32)
            tops = score(following, kb, tops)
        acc[rows_in, :] = total
        keep(tops)
        return carry

    lax.fori_loop(0, count, step, 0)
    if first:
        return
    for k in range(4):
        source = lax.rem(quarter + 4 - k, 4)
        for i in range(4):
            at = pl.multiple_of((source * 4 + xs[i]) * QT, QT)
            rows_in = pl.ds(at, QT)
            outs[i][k] = (acc[rows_in, :HD] / acc[rows_in, HD:]).astype(BF)


def attention(lengths, qs, mine, theirs, spread, given=()):
    first = not given
    anyspace = pl.BlockSpec(memory_space=pl.ANY)
    whole = pl.BlockSpec(memory_space=VMEM)
    state = [shape((2048, 2 * HD), F32), shape((2048, HD), F32)]
    working = [] if first else [pltpu.VMEM((2048, 2 * HD), F32), pltpu.VMEM((2048, HD), F32)]
    outs = state if first else [shape((4, QT, HD))] * 4
    return call(
        functools.partial(attention_body, spread, first),
        outs,
        [lengths, *qs, mine, theirs, *given],
        [
            *working,
            pltpu.VMEM((16, QT, HD), BF),
            pltpu.VMEM((4096, HD), BF),
            pltpu.VMEM((4096, 2 * HD), BF),
            pltpu.VMEM((4, 512, 512), F32),
            pltpu.VMEM((512, HD), F32),
            pltpu.SemaphoreType.DMA,
        ],
        in_specs=[pl.BlockSpec(memory_space=SMEM)] + [anyspace] * 6 + [whole] * len(given),
        out_specs=[whole] * len(outs),
        flops=3 << 30,
        size=8 << 20,
        limit=24 << 20,
    )


def project_body(gain, rows, *refs):
    mixed_in, ws = refs[:4], refs[4:9]
    after, top, low, total, mixed, acc = refs[9:]
    c, y, x, z = seats()
    for kk in range(4):
        z_from = lax.rem(y + 4 - kk, 4)
        for i, s in enumerate(SHIFTS):
            head = z_from * 4 + lax.rem(x + 4 - s, 4)
            mixed[:, pl.ds(pl.multiple_of(head * HD, HD), HD)] = mixed_in[kk][i]

    def step(n, carry):
        columns = pl.ds(pl.multiple_of(n * 512, 512), 512)

        def term(slab, offset, w):
            at = pl.multiple_of(lax.rem(slab, 4) * 512 + offset, 256)
            return jnp.dot(mixed[:, pl.ds(at, w.shape[0])], w[:, columns], preferred_element_type=F32)

        sums = term(z, 0, ws[0])
        sums = sums + term(z + 3 + 2 * c, 0, ws[1]) + term(z + 5 - 2 * c, 0, ws[2])
        sums = sums + term(z + 2, c * 256, ws[3]) + term(z + 2, (1 - c) * 256, ws[4])
        acc[:, columns] = sums
        return carry

    lax.fori_loop(0, 4, step, 0)
    rounded = (rows[...].astype(F32) + acc[...]).astype(BF)
    after[...] = rounded
    floats = rounded.astype(F32)
    normed2 = normalized(floats, gain[...])
    top[...] = normed2[: QT // 2]
    low[...] = normed2[QT // 2 :]
    total[...] = jnp.broadcast_to(jnp.sum(floats, axis=0, keepdims=True), (8, D))


def project(gain, rows, mixed_in, ws):
    return call(
        project_body,
        [shape((QT, D)), shape((QT // 2, D)), shape((QT // 2, D)), shape((8, D), F32)],
        [gain, rows, *mixed_in, *ws],
        [pltpu.VMEM((QT, D), BF), pltpu.VMEM((QT, D), F32)],
        flops=2 * QT * D * D,
        size=9 << 20,
        limit=PROJECT_LIMIT,
    )


def pack_body(*refs):
    out = refs[4]
    for i in range(4):
        out[i] = refs[i][...]


def pack(pieces):
    n = pieces[0].shape[0]
    return call(
        pack_body, shape((4, n, 2 * HD)), pieces, grid=(1,),
        in_specs=[pl.BlockSpec((n, 2 * HD), lambda i: (0, 0))] * 4,
        out_specs=pl.BlockSpec((4, n, 2 * HD), lambda i: (0, 0, 0)),
        flops=1 << 22, size=n << 12, limit=8 << 20,
    )


def share_body(*refs):
    out = refs[6]
    home = seats()[0] == lax.div(seats()[1], 2)
    for pick, when in ((0, home), (1, jnp.logical_not(home))):

        @pl.when(when)
        def _():
            at = 0
            for g in range(3):
                part = refs[2 * g + pick]
                out[:, at : at + part.shape[1], :] = part[...]
                at += part.shape[1]


def final_body(after, own, *refs):
    total = after[...].astype(F32) + own[...]
    for part in refs[:3]:
        total = total + part[...].astype(F32)
    refs[3][...] = total.astype(BF)


def queries_body(order, *refs):
    pieces, outs = refs[:12], refs[12:]
    _, y, _, z = seats()
    for k in range(4):
        turn = lax.rem(y + k + 4 - z, 4)
        for shift in range(4):
            group, part = order[shift]

            @pl.when(turn == shift)
            def _():
                for i in range(4):
                    outs[k][i] = pieces[group * 4 + i][part * QT : (part + 1) * QT, :]


def queries(groups, order):
    pieces = [piece for group in groups for piece in group]
    return call(
        functools.partial(queries_body, order), [shape((4, QT, HD))] * 4, pieces, grid=(1,),
        in_specs=[pl.BlockSpec((p.shape[0], HD), lambda i: (0, 2)) for p in pieces],
        out_specs=[pl.BlockSpec((4, QT, HD), lambda i: (0, 0, 0))] * 4,
        flops=1 << 22, size=1 << 20, limit=8 << 20,
    )


def heads_body(*refs):
    c, y, _, z = seats()
    quarter = 2 * lax.rem(y, 2) + c
    for kk in range(4):
        k = lax.rem(quarter + 8 - z - kk, 4)
        for i in range(4):
            refs[4 + kk][i] = refs[i][k]


def mlp_body(parts, cuts, *refs):
    rows, w_up, w_down = refs[:parts], refs[parts], refs[parts + 1]
    outs = refs[-4 - len(cuts) : -4]
    sums, inside, upper, acc = refs[-4:]
    n, block = inside.shape[0], upper.shape[1]
    at = 0
    for part in rows:
        inside[at : at + part.shape[0], :] = part[...]
        at += part.shape[0]
    acc[...] = jnp.zeros_like(acc)
    index = lax.broadcasted_iota(jnp.int32, (16, block), 0)

    def step(f, carry):
        span = pl.ds(pl.multiple_of(f * block, block), block)
        hidden = jnp.dot(inside[...], w_up[:, span], preferred_element_type=F32)
        up = jax.nn.gelu(hidden, approximate=True).astype(BF)
        upper[:n, :] = up
        extra = jnp.zeros((16, block), F32)
        for q in range(n // QT):
            whole = jnp.sum(up[q * QT : (q + 1) * QT, :].astype(F32), axis=0, keepdims=True)
            high = whole.astype(BF).astype(F32)
            extra = jnp.where(index == 2 * q, high, jnp.where(index == 2 * q + 1, whole - high, extra))
        upper[n:, :] = extra.astype(BF)
        acc[...] += jnp.dot(upper[...], w_down[span, :], preferred_element_type=F32)
        return carry

    lax.fori_loop(0, w_up.shape[1] // block, step, 0)
    at = 0
    for out in outs:
        out[...] = acc[at : at + out.shape[0], :].astype(out.dtype)
        at += out.shape[0]
    sums[...] = acc[n:, :]


def mlp(parts, w_up, w_down, cuts):
    n = sum(part.shape[0] for part in parts)
    return call(
        functools.partial(mlp_body, len(parts), cuts),
        [*(shape((size, D), kind) for size, kind in cuts), shape((16, D), F32)],
        [*parts, w_up, w_down],
        [pltpu.VMEM((n, D), BF), pltpu.VMEM((n + 16, 512), BF), pltpu.VMEM((n + 16, D), F32)],
        flops=4 * n * D * w_up.shape[1],
        size=17 << 20,
        limit=MLP_LIMIT,
    )


def half_body(w, out, sem):
    rows = pl.ds(pl.multiple_of(lax.axis_index("dp").astype(jnp.int32) * 256, 256), 256)
    copy = pltpu.make_async_copy(w.at[rows, :], out, sem)
    copy.start()
    copy.wait()


def totals_body(near, far, mine, after, out):
    z = seats()[3]
    own = mine[0:1, :] + mine[1:2, :] + after[0:1, :]
    parts = ((0, own), (3, near[0:1, :] + near[1:2, :]), (1, near[2:3, :] + near[3:4, :]), (2, far[0:1, :] + far[1:2, :]))
    for frame in range(2):
        total = jnp.zeros((1, D), F32)
        for shift, part in parts:
            total = total + part * jnp.where(lax.rem(z + shift, 4) // 2 == frame, 1.0, 0.0)
        out[frame : frame + 1, :] = total


def stack_body(*refs):
    for i in range(4):
        refs[4][i] = refs[i][...]


def sum_body(*refs):
    refs[4][...] = refs[0][...] + refs[1][...] + refs[2][...] + refs[3][...]


def states_body(lengths, near, above, below, far, gain, bias, weight, out, means, states):
    c, y, x, _ = seats()
    length = lengths[c]
    for array, ys in ((near, 0), (below, -1), (above, 1), (far, 2)):
        for i, s in enumerate(SHIFTS):
            at = lax.rem(y + 4 + ys, 4) * 4 + lax.rem(x + 4 + s, 4)
            means[at] = array[i] * (1.0 / TOK_FRAME)
    state = jnp.zeros((1, D), F32)
    for frame in range(FRAMES):
        mean = means[frame // 2, frame % 2 : frame % 2 + 1, :]
        gate = jax.nn.sigmoid(mean * gain[...] + bias[...])
        state = jnp.where(frame < length, gate * state + (1.0 - gate) * mean, state)
        states[frame : frame + 1, :] = state
    values = jnp.sum(states[...] * weight[...], axis=1, keepdims=True)
    index = lax.broadcasted_iota(jnp.int32, (FRAMES, HD), 0)
    out[...] = jnp.where(index < length, values, 0.0)


def advantages_body(lengths, mine, theirs, first, second):
    c, y, x, _ = seats()
    length, length_other = lengths[c], lengths[1 - c]
    index = lax.broadcasted_iota(jnp.int32, (FRAMES, HD), 0)

    def gap_of(values, size):
        final = jnp.sum(jnp.where(index == size - 1, values, 0.0), axis=0, keepdims=True)
        return jnp.where(index < size, final - values, 0.0)

    gap, gap_other = gap_of(mine[...], length), gap_of(theirs[...], length_other)
    count = (length + length_other).astype(F32)
    summed = lambda v: jnp.sum(v, axis=0, keepdims=True)
    mean = (summed(gap) + summed(gap_other)) / count
    centered = jnp.where(index < length, gap - mean, 0.0)
    centered_other = jnp.where(index < length_other, gap_other - mean, 0.0)
    variance = (summed(centered * centered) + summed(centered_other * centered_other)) / count
    scaled = jnp.where(index < length, centered * lax.rsqrt(variance + 1e-05), 0.0)
    at = (y * 4 + x) * 2
    lane = lax.broadcasted_iota(jnp.int32, (1, HD), 1)

    def picked(values):
        one, two = (summed(jnp.where(index == at + e, values, 0.0)) for e in (0, 1))
        return jnp.where(lane == 0, one, two)[:, :2]

    first[...] = picked(mine[...])
    second[...] = picked(scaled)


def local(tokens, attn_gain, w_qkv, w_out, mlp_gain, w_up, w_down, pool_gain, pool_bias, value_weight, valid_frames):
    rows = tokens[0]
    line = lambda v: v.reshape(1, D)

    from_left = moved(rows, "tensor", 1)
    from_right = moved(rows, "tensor", -1)
    far_top = moved(from_left[:64], "tensor", 1)
    far_low = moved(from_right[64:], "tensor", -1)
    groups = (((rows,), (0,)), ((from_left, from_right), (-1, 1)), ((far_top, far_low), (2,)))
    spread = tuple(shift for group in groups for shift in group[1])

    pa_pairs, pb_pairs = [], []
    for core in range(2):
        for yy in range(4):
            if yy // 2 == core:
                pa_pairs.append((flat(core, yy), flat(core, yy ^ 1)))
            else:
                pa_pairs.append((flat(core, yy), flat(1 - core, 3 - yy)))
                pb_pairs.append((flat(core, yy), flat(core, yy ^ 1)))
    swap = [(0, 1), (1, 0)]

    chunks, held, order = [], [], {}
    for g, (parts, shifts) in enumerate(groups):
        made = qkv_of(line(attn_gain), parts, w_qkv)
        got = [made[0], moved(made[1], "x", 1), moved(made[3], "x", -1), moved(made[2], "x", 2)]
        held.append(got)
        block = pack(got)
        pa = lax.ppermute(block, ("dp", "y"), pa_pairs)
        pb = lax.ppermute(pa, ("dp", "y"), pb_pairs)
        chunks.append((block, pa, pb))
        for p, shift in enumerate(shifts):
            order[shift % 4] = (g, p)
    qs = []
    for k, part in enumerate(queries(held, order)):
        pairs = []
        for core in range(2):
            for yy in range(4):
                j = (yy + k) % 4
                pairs.append((flat(core, yy), flat(j % 2, 2 * core + j // 2)))
        qs.append(lax.ppermute(part, ("dp", "y"), pairs))

    shared = []
    for b in range(2):
        mine = call(
            share_body, shape((4, 512, 2 * HD)), [chunk[b + i] for chunk in chunks for i in range(2)],
            flops=1 << 24, size=2 << 20, limit=10 << 20,
        )
        shared.append((mine, lax.ppermute(mine, "dp", swap)))
    state = attention(valid_frames, qs, *shared[0], spread)
    outs = attention(valid_frames, qs, *shared[1], spread, tuple(state))

    w_first, _, _ = lax.optimization_barrier((w_out, far_low, far_top))
    pairs = [(4 * core + zz, 4 * core + (zz + 1 - 2 * core) % 4) for core in range(2) for zz in range(4)]
    w_near = lax.ppermute(w_first, ("dp", "tensor"), pairs)
    w_half = call(
        half_body, shape((256, D)), [w_near], [pltpu.SemaphoreType.DMA],
        in_specs=[pl.BlockSpec(memory_space=pl.ANY)], flops=1 << 22, size=2 << 20, limit=4 << 20,
    )
    w_far = lax.ppermute(w_half, ("dp", "tensor"), pairs)
    ws = [w_out, w_near, lax.ppermute(w_near, "dp", swap), w_far, lax.ppermute(w_far, "dp", swap)]

    heads = [outs[0], moved(outs[1], "x", -1), moved(outs[2], "x", 1), moved(outs[3], "x", 2)]
    heads = call(heads_body, [shape((4, QT, HD))] * 4, heads, flops=1 << 22, size=1 << 20, limit=8 << 20)
    mixed_in = []
    for kk, part in enumerate(heads):
        pairs = []
        for core in range(2):
            for yy in range(4):
                for zz in range(4):
                    j = 2 * (yy % 2) + core
                    pairs.append((flat(core, yy, zz), flat(yy // 2, (zz + kk) % 4, j)))
        mixed_in.append(lax.ppermute(part, ("dp", "y", "tensor"), pairs))
    after, top, low, after_sum = project(line(mlp_gain), rows, mixed_in, ws)

    left_top = moved(top, "tensor", 1)
    right_low = moved(low, "tensor", -1)
    opposite_top = moved(left_top, "tensor", 1)
    opposite_low = moved(right_low, "tensor", -1)
    left_low = moved(low, "tensor", 1)
    right_top = moved(top, "tensor", -1)
    own_part, own_sums = mlp((top, low), w_up, w_down, ((128, F32),))
    far_part, far_sums = mlp((opposite_top, opposite_low), w_up, w_down, ((128, BF),))
    near_in = (left_top, left_low, right_top, right_low)
    for_left, for_right, near_sums = mlp(near_in, w_up, w_down, ((128, BF), (128, BF)))
    sum_far = moved(far_part, "tensor", 2)
    sum_one = moved(for_right, "tensor", 1)
    sum_two = moved(for_left, "tensor", -1)
    block = lambda n: pl.BlockSpec((n, D), lambda i: (i, 0))
    hidden = call(
        final_body, shape((QT, D)), [after, own_part, sum_one, sum_two, sum_far], grid=(2,),
        in_specs=[block(64)] * 5, out_specs=block(64), flops=1 << 20, size=3 << 20, limit=8 << 20,
    )

    totals = call(
        totals_body, shape((2, D), F32), [near_sums, far_sums, own_sums, after_sum], flops=1 << 16, size=1 << 19, limit=4 << 20,
    )
    rest = [moved(totals, "tensor", s) for s in (1, -1, 2)]
    totals = call(sum_body, shape((2, D), F32), [totals, *rest], flops=1 << 14, size=1 << 17, limit=4 << 20)
    rest = [moved(totals, "x", s) for s in (1, -1, 2)]
    over_x = call(stack_body, shape((4, 2, D), F32), [totals, *rest], flops=1 << 14, size=1 << 17, limit=4 << 20)
    below, above, across = (moved(over_x, "y", s) for s in (1, -1, 2))
    values = call(
        states_body,
        shape((FRAMES, HD), F32),
        [valid_frames, over_x, above, below, across, line(pool_gain), line(pool_bias), line(value_weight)],
        [pltpu.VMEM((16, 2, D), F32), pltpu.VMEM((FRAMES, D), F32)],
        in_specs=[pl.BlockSpec(memory_space=SMEM)] + [pl.BlockSpec(memory_space=VMEM)] * 7,
        flops=1 << 20,
        size=1 << 20,
        limit=8 << 20,
    )
    other_values = lax.ppermute(values, "dp", swap)
    frame_values, advantages = call(
        advantages_body,
        [shape((1, 2), F32)] * 2,
        [valid_frames, values, other_values],
        in_specs=[pl.BlockSpec(memory_space=SMEM)] + [pl.BlockSpec(memory_space=VMEM)] * 2,
        flops=1 << 14,
        size=1 << 15,
        limit=4 << 20,
    )
    return hidden[None], frame_values, advantages


def solution(mesh):
    fine = Mesh(mesh.devices.reshape(2, 4, 4, 4), ("dp", "y", "x", "tensor"))
    token_spec = P("dp", ("y", "x", "tensor"), None)
    in_specs = (
        token_spec,
        P(),
        P(None, None, "tensor"),
        P("tensor", None),
        P(),
        P(None, "tensor"),
        P("tensor", None),
        P(),
        P(),
        P(),
        P(),
    )
    out_specs = (token_spec, P("dp", ("y", "x")), P("dp", ("y", "x")))
    return jax.shard_map(local, mesh=fine, in_specs=in_specs, out_specs=out_specs, check_vma=False)
```
